8 devices in a mesh: dp: 4 (over z, y, x), tp: 2 (over core).
Axes of the slice: x: 2, y: 2, z: 1, core: 2. Of those that a mesh axis runs over, the one named last changes fastest.
Arguments:
- grad_qkv: bfloat16 [4, 1024, 4096], P('dp', None, 'tp')
- grad_o: bfloat16 [4, 2048, 1024], P('dp', 'tp')
- grad_gate: bfloat16 [4, 1024, 3072], P('dp', None, 'tp')
- grad_up: bfloat16 [4, 1024, 3072], P('dp', None, 'tp')
- grad_down: bfloat16 [4, 3072, 1024], P('dp', 'tp')
- w_qkv: float32 [1024, 4096], P(None, 'tp')
- w_o: float32 [2048, 1024], P('tp')
- w_gate: float32 [1024, 3072], P(None, 'tp')
- w_up: float32 [1024, 3072], P(None, 'tp')
- w_down: float32 [3072, 1024], P('tp')
- mom_qkv: float32 [1024, 4096], P(None, 'tp')
- mom_o: float32 [2048, 1024], P('tp')
- mom_gate: float32 [1024, 3072], P(None, 'tp')
- mom_up: float32 [1024, 3072], P(None, 'tp')
- mom_down: float32 [3072, 1024], P('tp')
Outputs:
- output 1: float32 [1024, 4096], P(None, 'tp')
- output 2: float32 [2048, 1024], P('tp')
- output 3: float32 [1024, 3072], P(None, 'tp')
- output 4: float32 [1024, 3072], P(None, 'tp')
- output 5: float32 [3072, 1024], P('tp')
- output 6: float32 [1024, 4096], P(None, 'tp')
- output 7: float32 [2048, 1024], P('tp')
- output 8: float32 [1024, 3072], P(None, 'tp')
- output 9: float32 [1024, 3072], P(None, 'tp')
- output 10: float32 [3072, 1024], P('tp')
All inputs are finite; a program needn't handle non-finite values.
Results may differ from the reference program's by a relative error of at most 0.02.
Values sent between devices are 32-bit elements.
A program may use at most 1 GiB of HBM per device.

```python
import math
import jax
import jax.numpy as jnp
from jax import lax

DP_SIZE = 4
D = 1024
HEADS = 16
KV_HEADS = 8
FF = 3072
HEAD_DIM = 128
NEWTON_STEPS = 5
GROUP_SIZE = HEADS // KV_HEADS
QKV_COLS = (HEADS + 2 * KV_HEADS) * HEAD_DIM
COEFF_A = 3.4445
COEFF_B = -4.7750
COEFF_C = 2.0315
MOMENTUM = 0.95
LEARN_RATE = 2e-3
WEIGHT_DECAY = 0.1
EPSILON = 1e-7


def draw_grad(base_key, arr_shape):
    row_count, col_count = arr_shape
    key_left, key_right, key_rows, key_cols, key_noise = jax.random.split(base_key, 5)
    rank_dim = 32
    left_factor = jax.random.normal(key_left, (DP_SIZE, row_count, rank_dim), jnp.float32)
    right_factor = jax.random.normal(key_right, (DP_SIZE, rank_dim, col_count), jnp.float32)
    row_scale = jnp.exp(0.5 * jax.random.normal(key_rows, (DP_SIZE, row_count, 1), jnp.float32))
    col_scale = jnp.exp(0.5 * jax.random.normal(key_cols, (DP_SIZE, 1, col_count), jnp.float32))
    noise_part = jax.random.normal(key_noise, (DP_SIZE, row_count, col_count), jnp.float32)
    low_rank = jnp.einsum('prk,pkc->prc', left_factor, right_factor) * (rank_dim ** -0.5)
    return ((low_rank + 0.5 * noise_part) * row_scale * col_scale).astype(jnp.bfloat16)


def setup_inputs(seed: int = 0) -> dict:
    key_list = jax.random.split(jax.random.key(seed), 15)
    arr_names = ['qkv', 'o', 'gate', 'up', 'down']
    arr_shapes = [(D, QKV_COLS), (HEADS * HEAD_DIM, D), (D, FF), (D, FF), (FF, D)]
    drawn = {}
    for arr_index in range(5):
        drawn['grad_' + arr_names[arr_index]] = draw_grad(key_list[arr_index], arr_shapes[arr_index])
    for arr_index in range(5):
        drawn['w_' + arr_names[arr_index]] = 5e-4 * jax.random.normal(key_list[5 + arr_index], arr_shapes[arr_index], jnp.float32)
    for arr_index in range(5):
        drawn['mom_' + arr_names[arr_index]] = (DP_SIZE ** -0.5) * jax.random.normal(key_list[10 + arr_index], arr_shapes[arr_index], jnp.float32)
    return drawn


def orthogonalize(mat_in):
    norm_val = jnp.sqrt(jnp.sum(mat_in * mat_in))
    start = (mat_in / (norm_val + EPSILON)).astype(jnp.bfloat16)

    def newton_step(x_cur, unused):
        gram = jnp.dot(x_cur, x_cur.T, preferred_element_type=jnp.float32)
        gram_half = gram.astype(jnp.bfloat16)
        poly_mat = COEFF_B * gram + COEFF_C * jnp.dot(gram_half, gram_half, preferred_element_type=jnp.float32)
        x_next = COEFF_A * x_cur.astype(jnp.float32) + jnp.dot(poly_mat.astype(jnp.bfloat16), x_cur, preferred_element_type=jnp.float32)
        return x_next.astype(jnp.bfloat16), None

    result, _ = lax.scan(newton_step, start, None, length=NEWTON_STEPS)
    return result


def scaled_update(x_orth):
    return 0.2 * math.sqrt(max(x_orth.shape[0], x_orth.shape[1])) * x_orth.astype(jnp.float32)


def momentum_pair(grads, mom_in):
    grad_avg = jnp.sum(grads.astype(jnp.float32), axis=0) / DP_SIZE
    mom_new = MOMENTUM * mom_in + grad_avg
    return mom_new, grad_avg + MOMENTUM * mom_new


def apply_step(weight, update):
    return weight - LEARN_RATE * (update + WEIGHT_DECAY * weight)


def reference(grad_qkv, grad_o, grad_gate, grad_up, grad_down, w_qkv, w_o, w_gate, w_up, w_down, mom_qkv, mom_o, mom_gate, mom_up, mom_down):
    mom_new_qkv, nest_qkv = momentum_pair(grad_qkv, mom_qkv)
    mom_new_o, nest_o = momentum_pair(grad_o, mom_o)
    mom_new_gate, nest_gate = momentum_pair(grad_gate, mom_gate)
    mom_new_up, nest_up = momentum_pair(grad_up, mom_up)
    mom_new_down, nest_down = momentum_pair(grad_down, mom_down)
    nest_split = nest_qkv.reshape(D, KV_HEADS, GROUP_SIZE + 2, HEAD_DIM)
    q_orth = orthogonalize(nest_split[:, :, :GROUP_SIZE, :].reshape(D, HEADS * HEAD_DIM))
    k_orth = orthogonalize(nest_split[:, :, GROUP_SIZE, :].reshape(D, KV_HEADS * HEAD_DIM))
    v_orth = orthogonalize(nest_split[:, :, GROUP_SIZE + 1, :].reshape(D, KV_HEADS * HEAD_DIM))
    upd_qkv = jnp.concatenate([
        scaled_update(q_orth).reshape(D, KV_HEADS, GROUP_SIZE, HEAD_DIM),
        scaled_update(k_orth).reshape(D, KV_HEADS, 1, HEAD_DIM),
        scaled_update(v_orth).reshape(D, KV_HEADS, 1, HEAD_DIM)], axis=2).reshape(D, QKV_COLS)
    upd_o = scaled_update(orthogonalize(nest_o.T)).T
    upd_gate = scaled_update(orthogonalize(nest_gate))
    upd_up = scaled_update(orthogonalize(nest_up))
    upd_down = scaled_update(orthogonalize(nest_down.T)).T
    return (apply_step(w_qkv, upd_qkv), apply_step(w_o, upd_o), apply_step(w_gate, upd_gate), apply_step(w_up, upd_up), apply_step(w_down, upd_down), mom_new_qkv, mom_new_o, mom_new_gate, mom_new_up, mom_new_down)
```

```python
import functools
import math
import jax
import jax.numpy as jnp
from jax import lax
from jax.experimental import pallas as pl
from jax.experimental.pallas import tpu as pltpu
from jax.sharding import PartitionSpec as P

HEAD_DIM = 128
NEWTON_STEPS = 5
COEFF_A = 3.4445
COEFF_B = -4.7750
COEFF_C = 2.0315
MOMENTUM = 0.95
LEARN_RATE = 2e-3
WEIGHT_DECAY = 0.1
EPSILON = 1e-7
PANEL = 512
VMEM_BYTES = 67043328
F32 = jnp.float32
BF16 = jnp.bfloat16


GROUP_COLS = 2 * HEAD_DIM
MESH = pl.DeviceIdType.MESH
PIECE_R = 128
PIECE_C = 512
HALF_R = PIECE_R // 2
QUART_R = PIECE_R // 4
DOWN, GATE_UP, O_Q, KEY_VALUE = range(4)
FIRST = (0, 12, 36, 52)
LAST = (12, 36, 52, 60)
PAIRS = 60


def ds(start, size):
    return pl.ds(start if isinstance(start, int) else pl.multiple_of(start, math.gcd(size, 128)), size)


def moved_momentum(grad, mom):
    mom_new = MOMENTUM * mom + grad
    return mom_new, grad + MOMENTUM * mom_new


def weight_step(weight, x_orth, scale):
    return weight - LEARN_RATE * (scale * x_orth + WEIGHT_DECAY * weight)


def gram_panel(x_ref, depth, j):
    return lax.dot_general(x_ref[:(j + 1) * PANEL, :depth], x_ref[j * PANEL:(j + 1) * PANEL, :depth], (((1,), (1,)), ((), ())),
                           preferred_element_type=F32)


def gram_step(x_ref, depth, s_ref, sb_ref, between=lambda: None):
    for j in range(s_ref.shape[0] // PANEL):
        cols = slice(j * PANEL, (j + 1) * PANEL)
        part = gram_panel(x_ref, depth, j)
        s_ref[:(j + 1) * PANEL, cols] = part
        half = part.astype(BF16)
        sb_ref[:(j + 1) * PANEL, cols] = half
        if j:
            sb_ref[cols, :j * PANEL] = half[:j * PANEL, :].T
        between()


def poly_step(s_ref, sb_ref, t_ref, between=lambda: None):
    for j in range(s_ref.shape[0] // PANEL):
        cols = slice(j * PANEL, (j + 1) * PANEL)
        part = jnp.dot(sb_ref[:(j + 1) * PANEL, :], sb_ref[:, cols], preferred_element_type=F32)
        poly_part = (COEFF_B * s_ref[:(j + 1) * PANEL, cols] + COEFF_C * part).astype(BF16)
        t_ref[:(j + 1) * PANEL, cols] = poly_part
        if j:
            t_ref[cols, :j * PANEL] = poly_part[:j * PANEL, :].T
        between()


def advanced(t_ref, x_ref, cols):
    x_cur = x_ref[:, cols]
    prod = jnp.dot(t_ref[...], x_cur, preferred_element_type=F32)
    return (COEFF_A * x_cur.astype(F32) + prod).astype(BF16)


def step_kernel(*refs):
    (g_qkv, g_o, g_gate, g_up, g_down, w_qkv, w_o, w_gate, w_up, w_down, m_qkv, m_o, m_gate, m_up, m_down,
     wn_qkv, wn_o, wn_gate, wn_up, wn_down, mn_qkv, mn_o, mn_gate, mn_up, mn_down, kv_out,
     nbuf, xbuf, s_ref, sb_ref, t_ref, xr, wrow, wcol, snd1, half, r1, r2, fin, gbuf, mbuf, mst, nst, nst_t,
     g_sem, m_sem, ms_sem, send1, send2, send3, send4, send5, recv1, recv2, recv3, recv4, recv5,
     nsend, dsend, nrecv, xsend, xrecv, wl_sem, ws_sem, kv_sem, credit) = refs
    dp = lax.axis_index('dp')
    core = lax.axis_index('tp')
    far = 1 - core
    pos_y, pos_x = lax.div(dp, 2), lax.rem(dp, 2)
    across = (pos_y * 2 + 1 - pos_x, (1 - pos_y) * 2 + pos_x)
    place = ((pos_x, pos_y), (pos_y, pos_x))
    d = s_ref.shape[0]

    def toward(k, second):
        return {'dp': across[k ^ second]}

    barrier = pltpu.get_barrier_semaphore()
    for where in ({'dp': across[0]}, {'dp': across[1]}, {'tp': far}):
        pl.semaphore_signal(barrier, inc=1, device_id=where, device_id_type=MESH)
    pl.semaphore_wait(barrier, 3)

    def blocks(phase, k, t, mats):
        j = t - FIRST[phase]
        qkv, o, gate, up, down = mats
        if phase == DOWN:
            return [(down.at[ds(j * PIECE_R, PIECE_R), pl.ds(k * PIECE_C, PIECE_C)], slice(0, PIECE_C))]
        if phase == GATE_UP:
            return [((gate, up)[k].at[ds(lax.div(j, 3) * PIECE_R, PIECE_R), ds(lax.rem(j, 3) * PIECE_C, PIECE_C)], slice(0, PIECE_C))]
        if phase == O_Q and k == 0:
            return [(o.at[ds(lax.div(j, 2) * PIECE_R, PIECE_R), ds(lax.rem(j, 2) * PIECE_C, PIECE_C)], slice(0, PIECE_C))]
        row, part, skip = (lax.div(j, 2), lax.rem(j, 2), 0) if phase == O_Q else (j, k, GROUP_COLS)
        return [(qkv.at[ds(row * PIECE_R, PIECE_R), ds(part * 4 * GROUP_COLS + skip + 2 * g * GROUP_COLS, GROUP_COLS)],
                 slice(g * GROUP_COLS, (g + 1) * GROUP_COLS)) for g in range(2)]

    def by_phase(t, low, high, phases, fn):
        for phase in phases:
            first, last = FIRST[phase], LAST[phase]
            if high < first or low >= last:
                continue
            if low >= first and high < last:
                fn(phase)
            else:
                pl.when((t >= first) & (t < last))(functools.partial(fn, phase))

    grads = (g_qkv, g_o, g_gate, g_up, g_down)
    moms = (m_qkv, m_o, m_gate, m_up, m_down)
    mom_news = (mn_qkv, mn_o, mn_gate, mn_up, mn_down)

    def waited(ref, sem):
        pltpu.make_async_copy(ref, ref, sem).wait()

    def load_grads(t, low, high):
        def start(phase):
            for k in range(2):
                for ref, cols in blocks(phase, k, t, grads):
                    pltpu.make_async_copy(ref, gbuf.at[lax.rem(t, 8), k, :, cols], g_sem.at[lax.rem(t, 8), k]).start()
        by_phase(t, low, high, range(4), start)

    def remote(src, dst, send, recv, where):
        return pltpu.make_async_remote_copy(src_ref=src, dst_ref=dst, send_sem=send, recv_sem=recv, device_id=where,
                                            device_id_type=MESH)

    def copies(k, t, which):
        s4, s8 = lax.rem(t, 4), lax.rem(t, 8)
        a, b = place[k]
        keep = ds(a * HALF_R + b * QUART_R, QUART_R)
        got = ds(a * HALF_R + (1 - b) * QUART_R, QUART_R)
        if which == 0:
            return remote(snd1.at[s4, k], r1.at[s8, k], send1.at[s4, k], recv1.at[s8, k], toward(k, 0))
        if which == 1:
            return remote(half.at[s4, k, ds((1 - b) * QUART_R, QUART_R)], r2.at[s8, k], send2.at[s4, k], recv2.at[s8, k], toward(k, 1))
        if which == 2:
            return remote(fin.at[s8, k, keep], fin.at[s8, k, keep], send3.at[s8, k], recv3.at[s8, k], toward(k, 1))
        if which == 3:
            return remote(fin.at[s8, k, keep], fin.at[s8, k, keep], send4.at[s8, k], recv4.at[s8, k], toward(k, 0))
        return remote(fin.at[s8, k, got], fin.at[s8, k, got], send5.at[s8, k], recv5.at[s8, k], toward(k, 0))

    def send_half(t, low, high):
        s4, s8 = lax.rem(t, 4), lax.rem(t, 8)
        for k in range(2):
            waited(gbuf.at[s8, k], g_sem.at[s8, k])
            a = place[k][0]
            snd1[s4, k] = gbuf[s8, k, ds((1 - a) * HALF_R, HALF_R), :].astype(F32)
            copies(k, t, 0).start()

    def send_quarter(t, low, high):
        s4, s8 = lax.rem(t, 4), lax.rem(t, 8)
        for k in range(2):
            copies(k, t, 0).wait()
            a = place[k][0]
            half[s4, k] = gbuf[s8, k, ds(a * HALF_R, HALF_R), :].astype(F32) + r1[s8, k]
            copies(k, t, 1).start()

    def share_quarter(t, low, high):
        s4, s8 = lax.rem(t, 4), lax.rem(t, 8)
        for k in range(2):
            copies(k, t, 1).wait()
            a, b = place[k]
            fin[s8, k, ds(a * HALF_R + b * QUART_R, QUART_R), :] = (half[s4, k, ds(b * QUART_R, QUART_R), :] + r2[s8, k]) * 0.25
            copies(k, t, 2).start()
            copies(k, t, 3).start()

    def pass_quarter(t, low, high):
        s4 = lax.rem(t, 4)
        for k in range(2):
            copies(k, t, 2).wait_recv()
            copies(k, t, 4).start()

        def start(phase):
            for k in range(2):
                for ref, cols in blocks(phase, k, t, moms):
                    pltpu.make_async_copy(ref, mbuf.at[s4, k, :, cols], m_sem.at[s4, k]).start()
        by_phase(t, low, high, range(3), start)

    def away_block(t, phase, k):
        j = t - FIRST[phase]
        s2 = lax.rem(t, 2)
        if phase == GATE_UP:
            src, rows, cols = nst.at[s2], ds(lax.div(j, 3) * PIECE_R, PIECE_R), ds(lax.rem(j, 3) * PIECE_C, PIECE_C)
        elif k == 0:
            src, rows, cols = nst_t.at[s2], ds(lax.rem(j, 2) * PIECE_C, PIECE_C), ds(lax.div(j, 2) * PIECE_R, PIECE_R)
        else:
            src, rows, cols = nst.at[s2], ds(lax.div(j, 2) * PIECE_R, PIECE_R), ds(lax.rem(j, 2) * PIECE_C, PIECE_C)
        return src, rows, cols

    def retire(t, low, high):
        s2, s4, s8 = lax.rem(t, 2), lax.rem(t, 4), lax.rem(t, 8)
        for k in range(2):
            copies(k, t, 2).wait_send()
            copies(k, t, 3).wait()
            copies(k, t, 4).wait()

        def finish(phase):
            if phase == KEY_VALUE:
                for k in range(2):
                    rows = ds((t - FIRST[KEY_VALUE]) * PIECE_R, PIECE_R)
                    pltpu.make_async_copy(fin.at[s8, k], kv_out.at[rows, pl.ds(k * PIECE_C, PIECE_C)], kv_sem).start()
                return
            if phase:
                @pl.when(t == FIRST[phase])
                def _():
                    pl.semaphore_wait(credit, 1)

                @pl.when(t > FIRST[phase])
                def _():
                    waited(nst.at[lax.rem(t + 1, 2)], nsend.at[lax.rem(t + 1, 2)])
            for k in range(2):
                waited(mbuf.at[s4, k], m_sem.at[s4, k])
                if phase:
                    waited(mst.at[s4, k], ms_sem.at[s4, k])
                else:
                    @pl.when(t >= 4)
                    def _():
                        waited(mst.at[s4, k], ms_sem.at[s4, k])
                mom_new, nest = moved_momentum(fin[s8, k], mbuf[s4, k])
                mst[s4, k] = mom_new
                for ref, cols in blocks(phase, k, t, mom_news):
                    pltpu.make_async_copy(mst.at[s4, k, :, cols], ref, ms_sem.at[s4, k]).start()
                if phase == DOWN:
                    rows, cols = pl.ds(k * PIECE_C, PIECE_C), ds(t * PIECE_R, PIECE_R)
                    nbuf[core, rows, cols] = nest.T
                    remote(nbuf.at[core, rows, cols], nbuf.at[core, rows, cols], dsend, nrecv.at[DOWN], {'tp': far}).start()
                    continue
                turned = phase == O_Q and k == 0
                piece = nest.T if turned else nest
                src, rows, cols = away_block(t, phase, k)

                @pl.when(core == k)
                def _():
                    nbuf[core, rows, cols] = piece

                @pl.when(core != k)
                def _():
                    (nst_t if turned else nst)[s2] = piece
                    remote(src, nbuf.at[core, rows, cols], nsend.at[s2], nrecv.at[phase], {'tp': far}).start()
        by_phase(t, low, high, range(4), finish)

    def service(s, low, high):
        for offset, stage in ((6, pass_quarter), (4, share_quarter), (2, send_quarter), (0, send_half), (8, retire), (-2, load_grads)):
            t, lo, hi = s - offset, low - offset, high - offset
            if hi < 0 or lo >= PAIRS:
                continue
            run = functools.partial(stage, t, max(lo, 0), min(hi, PAIRS - 1))
            if lo >= 0 and hi < PAIRS:
                run()
            else:
                pl.when((t >= 0) & (t < PAIRS))(run)

    def services(low, high):
        def one(s, carry):
            service(s, low, high)
            return carry
        lax.fori_loop(low, high + 1, one, 0)

    def newton(phase, w, scale, first_service):
        waited(nbuf.at[far, :, pl.ds(0, w)], nrecv.at[phase])
        if phase == DOWN:
            waited(nbuf.at[core, :, pl.ds(0, w)], dsend)
        else:
            end = (LAST[phase] - 1) % 2
            waited(nst.at[end], nsend.at[end])
        rows_step = 64

        def square_rows(r, acc):
            rows = ds(r * rows_step, rows_step)
            a = nbuf[core, rows, :w]
            b = nbuf[far, rows, :w]
            return acc + (a * a + b * b)

        acc = lax.fori_loop(0, d // rows_step, square_rows, jnp.zeros((rows_step, w), F32))
        inv = 1.0 / (jnp.sqrt(jnp.sum(acc)) + EPSILON)

        def fill_rows(r, carry):
            rows = ds(r * rows_step, rows_step)
            xbuf[rows, :w] = (nbuf[core, rows, :w] * inv).astype(BF16)
            xbuf[rows, w:2 * w] = (nbuf[far, rows, :w] * inv).astype(BF16)
            return carry

        lax.fori_loop(0, d // rows_step, fill_rows, 0)
        if phase < O_Q:
            pl.semaphore_signal(credit, inc=1, device_id={'tp': far}, device_id_type=MESH)

        def step(i, carry):
            gram_step(xbuf, 2 * w, s_ref, sb_ref)
            last = first_service + 2 * NEWTON_STEPS - 1
            service(first_service + 2 * i, first_service, last)
            poly_step(s_ref, sb_ref, t_ref)

            @pl.when(i < NEWTON_STEPS - 1)
            def _():
                def move(c, inner):
                    cols = ds(c * PANEL, PANEL)
                    xbuf[:, cols] = advanced(t_ref, xbuf, cols)
                    return inner
                lax.fori_loop(0, 2 * w // PANEL, move, 0)
            service(first_service + 2 * i + 1, first_service, last)
            return carry

        lax.fori_loop(0, NEWTON_STEPS, step, 0)
        count = w // PANEL
        if phase != DOWN:
            def return_copy(c):
                cols = slice((c % 2) * PANEL, (c % 2 + 1) * PANEL)
                return remote(s_ref.at[:, cols], xr.at[:, pl.ds(c * PANEL, PANEL)], xsend.at[c % 2], xrecv.at[phase], {'tp': far})

            for c in range(count):
                if c >= 2:
                    return_copy(c - 2).wait_send()
                s_ref[:, (c % 2) * PANEL:(c % 2 + 1) * PANEL] = advanced(t_ref, xbuf, pl.ds(w + c * PANEL, PANEL)).astype(F32)
                return_copy(c).start()

        def own(c, carry):
            cols = ds(c * PANEL, PANEL)
            xbuf[:, cols] = advanced(t_ref, xbuf, cols)
            return carry

        lax.fori_loop(0, count, own, 0)
        if phase != DOWN:
            for c in range(max(count - 2, 0), count):
                return_copy(c).wait_send()
            waited(xr.at[:, pl.ds(0, w)], xrecv.at[phase])

        def weights(k, weight, weight_new, kind):
            buf = wrow if kind == 'rows' else wcol
            count = w // 256

            def part(ref, i):
                if kind == 'rows':
                    return ref.at[ds(i * 256, 256), :]
                return ref.at[:, ds(i * (512 if kind == 'groups' else 256), 256)]

            def load(i):
                return pltpu.make_async_copy(part(weight, i), buf.at[lax.rem(i, 3)], wl_sem.at[lax.rem(i, 3)])

            def store(i):
                return pltpu.make_async_copy(buf.at[lax.rem(i, 3)], part(weight_new, i), ws_sem.at[lax.rem(i, 3)])

            load(jnp.int32(0)).start()
            load(jnp.int32(1)).start()

            def one(i, carry):
                cols = ds(i * 256, 256)
                slot = lax.rem(i, 3)
                load(i).wait()

                def put(x_orth):
                    buf[slot] = weight_step(buf[slot], x_orth.T if kind == 'rows' else x_orth, scale)

                if phase == DOWN:
                    put(xbuf[:, cols].astype(F32))
                else:
                    @pl.when(core == k)
                    def _():
                        put(xbuf[:, cols].astype(F32))

                    @pl.when(core != k)
                    def _():
                        put(xr[:, cols])
                store(i).start()

                @pl.when(i >= 1)
                def _():
                    store(i - 1).wait()

                @pl.when(i + 2 < count)
                def _():
                    load(i + 2).start()
                return carry

            lax.fori_loop(0, count, one, 0)
            store(jnp.int32(count - 1)).wait()

        return weights

    load_grads(jnp.int32(0), 0, 0)
    load_grads(jnp.int32(1), 1, 1)
    services(0, 19)
    w_long, w_mid = w_gate.shape[1], w_o.shape[0]

    def scale_of(w):
        return 0.2 * math.sqrt(max(d, 2 * w))

    weights = newton(DOWN, w_long, scale_of(w_long), 20)
    weights(0, w_down, wn_down, 'rows')
    services(30, 43)
    weights = newton(GATE_UP, w_long, scale_of(w_long), 44)
    weights(0, w_gate, wn_gate, 'cols')
    service(jnp.int32(54), 54, 54)
    weights(1, w_up, wn_up, 'cols')
    services(55, 59)
    weights = newton(O_Q, w_mid, scale_of(w_mid), 60)
    weights(0, w_o, wn_o, 'rows')
    weights(1, w_qkv, wn_qkv, 'groups')
    for t in range(LAST[O_Q] - 4, LAST[O_Q]):
        for k in range(2):
            waited(mst.at[t % 4, k], ms_sem.at[t % 4, k])
    waited(kv_out, kv_sem)


def main_step(grads, weights, moms):
    any_spec = pl.BlockSpec(memory_space=pl.ANY)
    ins = list(grads) + list(weights) + list(moms)
    d, width = weights[0].shape
    outs = [jax.ShapeDtypeStruct(a.shape, F32) for a in list(weights) + list(moms)] + [jax.ShapeDtypeStruct((d, width // 2), F32)]
    w_long = weights[2].shape[1]
    dma = pltpu.SemaphoreType.DMA
    pieces = (PIECE_R, PIECE_C)
    return pl.pallas_call(
        step_kernel,
        out_shape=outs,
        in_specs=[any_spec] * len(ins),
        out_specs=[any_spec] * len(outs),
        scratch_shapes=[
            pltpu.VMEM((2, d, w_long), F32), pltpu.VMEM((d, 2 * w_long), BF16), pltpu.VMEM((d, d), F32), pltpu.VMEM((d, d), BF16),
            pltpu.VMEM((d, d), BF16), pltpu.VMEM((d, w_long), F32), pltpu.VMEM((3, 256, d), F32), pltpu.VMEM((3, d, 256), F32),
            pltpu.VMEM((4, 2, HALF_R, PIECE_C), F32), pltpu.VMEM((4, 2, HALF_R, PIECE_C), F32),
            pltpu.VMEM((8, 2, HALF_R, PIECE_C), F32), pltpu.VMEM((8, 2, QUART_R, PIECE_C), F32), pltpu.VMEM((8, 2) + pieces, F32),
            pltpu.VMEM((8, 2) + pieces, BF16), pltpu.VMEM((4, 2) + pieces, F32), pltpu.VMEM((4, 2) + pieces, F32),
            pltpu.VMEM((2,) + pieces, F32), pltpu.VMEM((2, PIECE_C, PIECE_R), F32),
            dma((8, 2)), dma((4, 2)), dma((4, 2)), dma((4, 2)), dma((4, 2)), dma((8, 2)), dma((8, 2)), dma((8, 2)),
            dma((8, 2)), dma((8, 2)), dma((8, 2)), dma((8, 2)), dma((8, 2)),
            dma((2,)), dma, dma((3,)), dma((2,)), dma((3,)), dma((3,)), dma((3,)), dma, pltpu.SemaphoreType.REGULAR],
        compiler_params=pltpu.CompilerParams(vmem_limit_bytes=VMEM_BYTES, collective_id=0, has_side_effects=True),
        cost_estimate=pl.CostEstimate(flops=10 ** 11, bytes_accessed=2 * 10 ** 8, transcendentals=0),
    )(*ins)


def call(body, grid, ins, in_specs, outs, out_specs, aliases=None):
    moved = sum(math.prod(a.shape) * a.dtype.itemsize for a in jax.tree.leaves((ins, outs)))
    return pl.pallas_call(
        body, grid=grid, out_shape=outs, in_specs=in_specs, out_specs=out_specs,
        input_output_aliases=aliases or {},
        compiler_params=pltpu.CompilerParams(vmem_limit_bytes=VMEM_BYTES),
        cost_estimate=pl.CostEstimate(flops=moved, bytes_accessed=moved, transcendentals=0),
    )(*ins)


def momentum_kv(grad, mom):
    rows, width = grad.shape
    odd = pl.BlockSpec((rows, GROUP_COLS), lambda g: (0, 2 * g + 1))
    block = pl.BlockSpec((rows, GROUP_COLS), lambda g: (0, g))
    head = pl.BlockSpec((rows, HEAD_DIM), lambda g: (0, g))

    def body(t_ref, m_ref, mn_ref, own_ref, away_ref):
        mn, nest = moved_momentum(t_ref[...], m_ref[...])
        mn_ref[...] = mn
        first = lax.axis_index('tp') == 0
        key, value = nest[:, :HEAD_DIM], nest[:, HEAD_DIM:]
        own_ref[...] = jnp.where(first, key, value)
        away_ref[...] = jnp.where(first, value, key)

    part = jax.ShapeDtypeStruct((rows, width // 2), F32)
    return call(body, (width // GROUP_COLS,), (grad, mom), [block, odd],
                [jax.ShapeDtypeStruct(grad.shape, F32), part, part], [block, head, head])


def update_kv(weight, x_own, x_back, weight_new, scale):
    rows, width = x_own.shape
    odd = pl.BlockSpec((rows, GROUP_COLS), lambda g: (0, 2 * g + 1))
    head = pl.BlockSpec((rows, HEAD_DIM), lambda g: (0, g))

    def body(w_ref, own_ref, back_ref, unused, o_ref):
        first = lax.axis_index('tp') == 0
        own, back = own_ref[...], back_ref[...]
        o_ref[:, :HEAD_DIM] = weight_step(w_ref[:, :HEAD_DIM], jnp.where(first, own, back), scale)
        o_ref[:, HEAD_DIM:] = weight_step(w_ref[:, HEAD_DIM:], jnp.where(first, back, own), scale)

    return call(body, (width // HEAD_DIM,), (weight, x_own, x_back, weight_new),
                [odd, head, head, pl.BlockSpec(memory_space=pl.ANY)],
                jax.ShapeDtypeStruct(weight.shape, F32), odd, {3: 0})


PARTS = 4


def finish_kernel(*refs):
    own_ref, far_ref = refs[:2]
    srcs, kv_src = refs[2:12], refs[12]
    out_own, out_far = refs[13:15]
    dsts = refs[15:25]
    x_ref, s_ref, sb_ref, t_ref = refs[25:29]
    bufs = refs[29:39]
    in_sem, out_sem = refs[39:]
    d, w = own_ref.shape
    rows_step = 128

    def fetch(n, i):
        rows = srcs[n].shape[0] // PARTS
        at = ds(i * rows, rows)
        if n != 5:
            return [pltpu.make_async_copy(srcs[n].at[at, :], bufs[n], in_sem.at[n])]
        moves = []
        for g in range(srcs[n].shape[1] // (2 * GROUP_COLS)):
            lo = 2 * g * GROUP_COLS
            moves.append(pltpu.make_async_copy(srcs[n].at[at, lo:lo + GROUP_COLS], bufs[n].at[:, lo:lo + GROUP_COLS], in_sem.at[n]))
            moves.append(pltpu.make_async_copy(kv_src.at[at, g * GROUP_COLS:(g + 1) * GROUP_COLS],
                                               bufs[n].at[:, lo + GROUP_COLS:lo + 2 * GROUP_COLS], in_sem.at[n]))
        return moves

    def put(n, i):
        rows = srcs[n].shape[0] // PARTS
        return pltpu.make_async_copy(bufs[n], dsts[n].at[ds(i * rows, rows), :], out_sem.at[n])

    def fetch_at(n, i):
        @pl.when((i > 0) & (i < PARTS))
        def _():
            put(n, i - 1).wait()

        @pl.when(i < PARTS)
        def _():
            for move in fetch(n, i):
                move.start()

    def put_at(n, i):
        @pl.when(i < PARTS)
        def _():
            pltpu.make_async_copy(bufs[n], bufs[n], in_sem.at[n]).wait()
            put(n, i).start()

    def square_rows(r, acc):
        rows = ds(r * rows_step, rows_step)
        a = own_ref[rows, :]
        b = far_ref[rows, :]
        return acc + (a * a + b * b)

    acc = lax.fori_loop(0, d // rows_step, square_rows, jnp.zeros((rows_step, w), F32))
    inv = 1.0 / (jnp.sqrt(jnp.sum(acc)) + EPSILON)

    def fill_rows(r, carry):
        rows = ds(r * rows_step, rows_step)
        x_ref[rows, :w] = (own_ref[rows, :] * inv).astype(BF16)
        x_ref[rows, w:] = (far_ref[rows, :] * inv).astype(BF16)
        return carry

    lax.fori_loop(0, d // rows_step, fill_rows, 0)

    def step(i, carry):
        order = iter(((((0, 5), ()), ((1, 6), ()), ((2, 7), (0, 5)), ((3, 8), (1, 6)), ((4, 9), (2, 7)))))

        def between():
            starts, ends = next(order)
            for n in starts:
                fetch_at(n, i)
            for n in ends:
                put_at(n, i)

        between()
        gram_step(x_ref, 2 * w, s_ref, sb_ref, between)
        poly_step(s_ref, sb_ref, t_ref, between)

        @pl.when(i < NEWTON_STEPS - 1)
        def _():
            def move(c, inner):
                cols = ds(c * PANEL, PANEL)
                x_ref[:, cols] = advanced(t_ref, x_ref, cols)
                return inner
            lax.fori_loop(0, 2 * w // PANEL, move, 0)
        for n in (3, 8, 4, 9):
            put_at(n, i)
        return carry

    lax.fori_loop(0, NEWTON_STEPS, step, 0)
    for c in range(w // PANEL):
        cols = slice(c * PANEL, (c + 1) * PANEL)
        out_far[:, cols] = advanced(t_ref, x_ref, pl.ds(w + c * PANEL, PANEL)).astype(F32)
        out_own[:, cols] = advanced(t_ref, x_ref, pl.ds(c * PANEL, PANEL)).astype(F32)
    for n in range(10):
        put(n, PARTS - 1).wait()


def finish(own, far, arrays, mom_kv):
    d, w = own.shape
    any_spec = pl.BlockSpec(memory_space=pl.ANY)
    vmem = pl.BlockSpec(memory_space=pltpu.VMEM)
    dma = pltpu.SemaphoreType.DMA
    half = jax.ShapeDtypeStruct((d, w), F32)
    return pl.pallas_call(
        finish_kernel,
        out_shape=[half, half] + [jax.ShapeDtypeStruct(a.shape, F32) for a in arrays],
        in_specs=[vmem, vmem] + [any_spec] * (len(arrays) + 1),
        out_specs=[vmem, vmem] + [any_spec] * len(arrays),
        scratch_shapes=[pltpu.VMEM((d, 2 * w), BF16), pltpu.VMEM((d, d), F32), pltpu.VMEM((d, d), BF16), pltpu.VMEM((d, d), BF16)]
        + [pltpu.VMEM((a.shape[0] // PARTS, a.shape[1]), F32) for a in arrays] + [dma((10,)), dma((10,))],
        compiler_params=pltpu.CompilerParams(vmem_limit_bytes=VMEM_BYTES),
        cost_estimate=pl.CostEstimate(flops=3 * 10 ** 10, bytes_accessed=12 * 10 ** 7, transcendentals=0),
    )(own, far, *arrays, mom_kv)


def solution(mesh):
    tp_count = mesh.shape['tp']
    col_spec = P(None, 'tp')
    row_spec = P('tp', None)
    grad_col = P('dp', None, 'tp')
    grad_row = P('dp', 'tp', None)
    weight_specs = (col_spec, row_spec, col_spec, col_spec, row_spec)
    in_specs = (grad_col, grad_row, grad_col, grad_col, grad_row) + weight_specs + weight_specs
    out_specs = weight_specs + weight_specs
    swap = [(0, 1), (1, 0)]

    def local_step(*arrays):
        weights, moms = arrays[5:10], arrays[10:]
        results = main_step([block[0] for block in arrays[:5]], weights, moms)
        arrays, grad_kv = results[:10], results[10]
        mom_kv, own, away = momentum_kv(grad_kv, moms[0])
        done = finish(own, lax.ppermute(away, 'tp', swap), arrays, mom_kv)
        x_own, x_far, done = done[0], done[1], list(done[2:])
        scale = 0.2 * math.sqrt(max(own.shape[0], own.shape[1] * tp_count))
        done[0] = update_kv(weights[0], x_own, lax.ppermute(x_far, 'tp', swap), done[0], scale)
        return tuple(done)

    return jax.shard_map(local_step, mesh=mesh, in_specs=in_specs, out_specs=out_specs, check_vma=False)
```

```python
import functools
import math
import jax
import jax.numpy as jnp
from jax import lax
from jax.experimental import pallas as pl
from jax.experimental.pallas import tpu as pltpu
from jax.sharding import PartitionSpec as P

HEAD_DIM = 128
NEWTON_STEPS = 5
COEFF_A = 3.4445
COEFF_B = -4.7750
COEFF_C = 2.0315
MOMENTUM = 0.95
LEARN_RATE = 2e-3
WEIGHT_DECAY = 0.1
EPSILON = 1e-7
PANEL = 512
VMEM_BYTES = 67043328
F32 = jnp.float32
BF16 = jnp.bfloat16


GROUP_COLS = 2 * HEAD_DIM
MESH = pl.DeviceIdType.MESH
PIECE_R = 128
PIECE_C = 512
HALF_R = PIECE_R // 2
QUART_R = PIECE_R // 4
DOWN, GATE_UP, O_Q, KEY_VALUE = range(4)
KV_DELAY = 5
FIRST = (0, 12, 36, 52 + KV_DELAY)
LAST = (12, 36, 52, 60 + KV_DELAY)
PAIRS = LAST[-1]
BLOCK = 256


def ds(start, size):
    return pl.ds(start if isinstance(start, int) else pl.multiple_of(start, math.gcd(size, 128)), size)


def moved_momentum(grad, mom):
    mom_new = MOMENTUM * mom + grad
    return mom_new, grad + MOMENTUM * mom_new


def weight_step(weight, x_orth, scale):
    return weight - LEARN_RATE * (scale * x_orth + WEIGHT_DECAY * weight)


def gram_panel(x_ref, depth, j):
    return lax.dot_general(x_ref[:(j + 1) * BLOCK, :depth], x_ref[j * BLOCK:(j + 1) * BLOCK, :depth], (((1,), (1,)), ((), ())),
                           preferred_element_type=F32)


def gram_step(x_ref, depth, s_ref, sb_ref, between=lambda: None):
    for j in range(s_ref.shape[0] // BLOCK):
        cols = slice(j * BLOCK, (j + 1) * BLOCK)
        part = gram_panel(x_ref, depth, j)
        s_ref[:(j + 1) * BLOCK, cols] = part
        half = part.astype(BF16)
        sb_ref[:(j + 1) * BLOCK, cols] = half
        if j:
            sb_ref[cols, :j * BLOCK] = half[:j * BLOCK, :].T
        between()


def poly_step(s_ref, sb_ref, t_ref, between=lambda: None):
    for j in range(s_ref.shape[0] // BLOCK):
        cols = slice(j * BLOCK, (j + 1) * BLOCK)
        part = jnp.dot(sb_ref[:(j + 1) * BLOCK, :], sb_ref[:, cols], preferred_element_type=F32)
        poly_part = (COEFF_B * s_ref[:(j + 1) * BLOCK, cols] + COEFF_C * part).astype(BF16)
        t_ref[:(j + 1) * BLOCK, cols] = poly_part
        if j:
            t_ref[cols, :j * BLOCK] = poly_part[:j * BLOCK, :].T
        between()


def advanced(t_ref, x_ref, cols):
    x_cur = x_ref[:, cols]
    prod = jnp.dot(t_ref[...], x_cur, preferred_element_type=F32)
    return (COEFF_A * x_cur.astype(F32) + prod).astype(BF16)


def step_kernel(*refs):
    (g_qkv, g_o, g_gate, g_up, g_down, w_qkv, w_o, w_gate, w_up, w_down, m_qkv, m_o, m_gate, m_up, m_down,
     wn_qkv, wn_o, wn_gate, wn_up, wn_down, mn_qkv, mn_o, mn_gate, mn_up, mn_down, kv_out,
     nbuf, xbuf, s_ref, sb_ref, t_ref, xr, wrow, wcol, snd1, half, r1, r2, fin, gbuf, mbuf, mst, nst, nst_t,
     g_sem, m_sem, ms_sem, send1, send2, send3, send4, send5, recv1, recv2, recv3, recv4, recv5,
     nsend, dsend, nrecv, xsend, xrecv, wl_sem, ws_sem, kv_sem, credit) = refs
    dp = lax.axis_index('dp')
    core = lax.axis_index('tp')
    far = 1 - core
    pos_y, pos_x = lax.div(dp, 2), lax.rem(dp, 2)
    across = (pos_y * 2 + 1 - pos_x, (1 - pos_y) * 2 + pos_x)
    place = ((pos_x, pos_y), (pos_y, pos_x))
    d = s_ref.shape[0]

    def toward(k, second):
        return {'dp': across[k ^ second]}

    barrier = pltpu.get_barrier_semaphore()
    for where in ({'dp': across[0]}, {'dp': across[1]}, {'tp': far}):
        pl.semaphore_signal(barrier, inc=1, device_id=where, device_id_type=MESH)
    pl.semaphore_wait(barrier, 3)

    def blocks(phase, k, t, mats):
        j = t - FIRST[phase]
        qkv, o, gate, up, down = mats
        if phase == DOWN:
            return [(down.at[ds(j * PIECE_R, PIECE_R), pl.ds(k * PIECE_C, PIECE_C)], slice(0, PIECE_C))]
        if phase == GATE_UP:
            return [((gate, up)[k].at[ds(lax.div(j, 3) * PIECE_R, PIECE_R), ds(lax.rem(j, 3) * PIECE_C, PIECE_C)], slice(0, PIECE_C))]
        if phase == O_Q and k == 0:
            return [(o.at[ds(lax.div(j, 2) * PIECE_R, PIECE_R), ds(lax.rem(j, 2) * PIECE_C, PIECE_C)], slice(0, PIECE_C))]
        row, part, skip = (lax.div(j, 2), lax.rem(j, 2), 0) if phase == O_Q else (j, k, GROUP_COLS)
        return [(qkv.at[ds(row * PIECE_R, PIECE_R), ds(part * 4 * GROUP_COLS + skip + 2 * g * GROUP_COLS, GROUP_COLS)],
                 slice(g * GROUP_COLS, (g + 1) * GROUP_COLS)) for g in range(2)]

    def by_phase(t, low, high, phases, fn):
        for phase in phases:
            first, last = FIRST[phase], LAST[phase]
            if high < first or low >= last:
                continue
            if low >= first and high < last:
                fn(phase)
            else:
                pl.when((t >= first) & (t < last))(functools.partial(fn, phase))

    grads = (g_qkv, g_o, g_gate, g_up, g_down)
    moms = (m_qkv, m_o, m_gate, m_up, m_down)
    mom_news = (mn_qkv, mn_o, mn_gate, mn_up, mn_down)

    def waited(ref, sem):
        pltpu.make_async_copy(ref, ref, sem).wait()

    def load_grads(t, low, high):
        def start(phase):
            for k in range(2):
                for ref, cols in blocks(phase, k, t, grads):
                    pltpu.make_async_copy(ref, gbuf.at[lax.rem(t, 8), k, :, cols], g_sem.at[lax.rem(t, 8), k]).start()
        by_phase(t, low, high, range(4), start)

    def remote(src, dst, send, recv, where):
        return pltpu.make_async_remote_copy(src_ref=src, dst_ref=dst, send_sem=send, recv_sem=recv, device_id=where,
                                            device_id_type=MESH)

    def copies(k, t, which):
        s4, s8 = lax.rem(t, 4), lax.rem(t, 8)
        a, b = place[k]
        keep = ds(a * HALF_R + b * QUART_R, QUART_R)
        got = ds(a * HALF_R + (1 - b) * QUART_R, QUART_R)
        if which == 0:
            return remote(snd1.at[s4, k], r1.at[s8, k], send1.at[s4, k], recv1.at[s8, k], toward(k, 0))
        if which == 1:
            return remote(half.at[s4, k, ds((1 - b) * QUART_R, QUART_R)], r2.at[s8, k], send2.at[s4, k], recv2.at[s8, k], toward(k, 1))
        if which == 2:
            return remote(fin.at[s8, k, keep], fin.at[s8, k, keep], send3.at[s8, k], recv3.at[s8, k], toward(k, 1))
        if which == 3:
            return remote(fin.at[s8, k, keep], fin.at[s8, k, keep], send4.at[s8, k], recv4.at[s8, k], toward(k, 0))
        return remote(fin.at[s8, k, got], fin.at[s8, k, got], send5.at[s8, k], recv5.at[s8, k], toward(k, 0))

    def send_half(t, low, high):
        s4, s8 = lax.rem(t, 4), lax.rem(t, 8)
        for k in range(2):
            waited(gbuf.at[s8, k], g_sem.at[s8, k])
            a = place[k][0]
            snd1[s4, k] = gbuf[s8, k, ds((1 - a) * HALF_R, HALF_R), :].astype(F32)
            copies(k, t, 0).start()

    def send_quarter(t, low, high):
        s4, s8 = lax.rem(t, 4), lax.rem(t, 8)
        for k in range(2):
            copies(k, t, 0).wait()
            a = place[k][0]
            half[s4, k] = gbuf[s8, k, ds(a * HALF_R, HALF_R), :].astype(F32) + r1[s8, k]
            copies(k, t, 1).start()

    def share_quarter(t, low, high):
        s4, s8 = lax.rem(t, 4), lax.rem(t, 8)
        for k in range(2):
            copies(k, t, 1).wait()
            a, b = place[k]
            fin[s8, k, ds(a * HALF_R + b * QUART_R, QUART_R), :] = (half[s4, k, ds(b * QUART_R, QUART_R), :] + r2[s8, k]) * 0.25
            copies(k, t, 2).start()
            copies(k, t, 3).start()

    def pass_quarter(t, low, high):
        s4 = lax.rem(t, 4)
        for k in range(2):
            copies(k, t, 2).wait_recv()
            copies(k, t, 4).start()

        def start(phase):
            for k in range(2):
                for ref, cols in blocks(phase, k, t, moms):
                    pltpu.make_async_copy(ref, mbuf.at[s4, k, :, cols], m_sem.at[s4, k]).start()
        by_phase(t, low, high, range(4), start)

    def away_block(t, phase, k):
        j = t - FIRST[phase]
        s2 = lax.rem(t, 2)
        if phase == GATE_UP:
            src, rows, cols = nst.at[s2], ds(lax.div(j, 3) * PIECE_R, PIECE_R), ds(lax.rem(j, 3) * PIECE_C, PIECE_C)
        elif k == 0:
            src, rows, cols = nst_t.at[s2], ds(lax.rem(j, 2) * PIECE_C, PIECE_C), ds(lax.div(j, 2) * PIECE_R, PIECE_R)
        else:
            src, rows, cols = nst.at[s2], ds(lax.div(j, 2) * PIECE_R, PIECE_R), ds(lax.rem(j, 2) * PIECE_C, PIECE_C)
        return src, rows, cols

    def retire(t, low, high):
        s2, s4, s8 = lax.rem(t, 2), lax.rem(t, 4), lax.rem(t, 8)
        for k in range(2):
            copies(k, t, 2).wait_send()
            copies(k, t, 3).wait()
            copies(k, t, 4).wait()

        def finish(phase):
            if phase:
                @pl.when(t == FIRST[phase])
                def _():
                    pl.semaphore_wait(credit, 1)

                @pl.when(t > FIRST[phase])
                def _():
                    waited(nst.at[lax.rem(t + 1, 2)], nsend.at[lax.rem(t + 1, 2)])
            for k in range(2):
                waited(mbuf.at[s4, k], m_sem.at[s4, k])
                if phase:
                    waited(mst.at[s4, k], ms_sem.at[s4, k])
                else:
                    @pl.when(t >= 4)
                    def _():
                        waited(mst.at[s4, k], ms_sem.at[s4, k])
                mom_new, nest = moved_momentum(fin[s8, k], mbuf[s4, k])
                mst[s4, k] = mom_new
                for ref, cols in blocks(phase, k, t, mom_news):
                    pltpu.make_async_copy(mst.at[s4, k, :, cols], ref, ms_sem.at[s4, k]).start()
                if phase == DOWN:
                    rows, cols = pl.ds(k * PIECE_C, PIECE_C), ds(t * PIECE_R, PIECE_R)
                    nbuf[core, rows, cols] = nest.T
                    remote(nbuf.at[core, rows, cols], nbuf.at[core, rows, cols], dsend, nrecv.at[DOWN], {'tp': far}).start()
                    continue
                if phase == KEY_VALUE:
                    rows = ds((t - FIRST[KEY_VALUE]) * PIECE_R, PIECE_R)

                    def split(mine, nest=nest, k=k):
                        for g in range(2):
                            cols = slice((2 * k + g) * HEAD_DIM, (2 * k + g + 1) * HEAD_DIM)
                            heads = [nest[:, (2 * g + h) * HEAD_DIM:(2 * g + h + 1) * HEAD_DIM] for h in range(2)]
                            nbuf[core, rows, cols] = heads[mine]
                            nst[s2, :, cols] = heads[1 - mine]
                    pl.when(core == 0)(functools.partial(split, 0))
                    pl.when(core == 1)(functools.partial(split, 1))
                    if k:
                        remote(nst.at[s2], nbuf.at[core, rows, pl.ds(0, 2 * GROUP_COLS)], nsend.at[s2], nrecv.at[phase], {'tp': far}).start()
                    continue
                turned = phase == O_Q and k == 0
                piece = nest.T if turned else nest
                src, rows, cols = away_block(t, phase, k)

                @pl.when(core == k)
                def _():
                    nbuf[core, rows, cols] = piece

                @pl.when(core != k)
                def _():
                    (nst_t if turned else nst)[s2] = piece
                    remote(src, nbuf.at[core, rows, cols], nsend.at[s2], nrecv.at[phase], {'tp': far}).start()
        by_phase(t, low, high, range(4), finish)

    def service(s, low, high):
        for offset, stage in ((6, pass_quarter), (4, share_quarter), (2, send_quarter), (0, send_half), (8, retire), (-2, load_grads)):
            t, lo, hi = s - offset, low - offset, high - offset
            if hi < 0 or lo >= PAIRS:
                continue
            run = functools.partial(stage, t, max(lo, 0), min(hi, PAIRS - 1))
            guards = []
            if lo < 0:
                guards.append(t >= 0)
            if hi >= PAIRS:
                guards.append(t < PAIRS)
            if KV_DELAY and lo < FIRST[KEY_VALUE] and hi >= LAST[O_Q]:
                if lo >= LAST[O_Q] and hi < FIRST[KEY_VALUE]:
                    continue
                guards.append((t - LAST[O_Q]) * (t - FIRST[KEY_VALUE] + 1) > 0)
            if guards:
                pl.when(functools.reduce(jnp.logical_and, guards))(run)
            else:
                run()

    def services(low, high):
        def one(s, carry):
            service(s, low, high)
            return carry
        lax.fori_loop(low, high + 1, one, 0)

    def normalize(phase, w, x_out):
        waited(nbuf.at[far, :, pl.ds(0, w)], nrecv.at[phase])
        if phase == DOWN:
            waited(nbuf.at[core, :, pl.ds(0, w)], dsend)
        else:
            end = (LAST[phase] - 1) % 2
            waited(nst.at[end], nsend.at[end])
        rows_step = 64

        def square_rows(r, acc):
            rows = ds(r * rows_step, rows_step)
            a = nbuf[core, rows, :w]
            b = nbuf[far, rows, :w]
            return acc + (a * a + b * b)

        acc = lax.fori_loop(0, d // rows_step, square_rows, jnp.zeros((rows_step, w), F32))
        inv = 1.0 / (jnp.sqrt(jnp.sum(acc)) + EPSILON)

        def fill_rows(r, carry):
            rows = ds(r * rows_step, rows_step)
            x_out[rows, :w] = (nbuf[core, rows, :w] * inv).astype(BF16)
            x_out[rows, w:2 * w] = (nbuf[far, rows, :w] * inv).astype(BF16)
            return carry

        lax.fori_loop(0, d // rows_step, fill_rows, 0)

    def newton(phase, w, scale, first_service):
        normalize(phase, w, xbuf)
        pl.semaphore_signal(credit, inc=1, device_id={'tp': far}, device_id_type=MESH)

        def step(i, carry):
            gram_step(xbuf, 2 * w, s_ref, sb_ref)
            last = first_service + 2 * NEWTON_STEPS - 1
            service(first_service + 2 * i, first_service, last)
            poly_step(s_ref, sb_ref, t_ref)

            @pl.when(i < NEWTON_STEPS - 1)
            def _():
                def move(c, inner):
                    cols = ds(c * PANEL, PANEL)
                    xbuf[:, cols] = advanced(t_ref, xbuf, cols)
                    return inner
                lax.fori_loop(0, 2 * w // PANEL, move, 0)
            service(first_service + 2 * i + 1, first_service, last)
            return carry

        lax.fori_loop(0, NEWTON_STEPS, step, 0)
        count = w // PANEL
        if phase != DOWN:
            def return_copy(c):
                cols = slice((c % 2) * PANEL, (c % 2 + 1) * PANEL)
                return remote(s_ref.at[:, cols], xr.at[:, pl.ds(c * PANEL, PANEL)], xsend.at[c % 2], xrecv.at[phase], {'tp': far})

            for c in range(count):
                if c >= 2:
                    return_copy(c - 2).wait_send()
                s_ref[:, (c % 2) * PANEL:(c % 2 + 1) * PANEL] = advanced(t_ref, xbuf, pl.ds(w + c * PANEL, PANEL)).astype(F32)
                return_copy(c).start()

        def own(c, carry):
            cols = ds(c * PANEL, PANEL)
            xbuf[:, cols] = advanced(t_ref, xbuf, cols)
            return carry

        lax.fori_loop(0, count, own, 0)
        if phase != DOWN:
            for c in range(max(count - 2, 0), count):
                return_copy(c).wait_send()
            waited(xr.at[:, pl.ds(0, w)], xrecv.at[phase])

        def weights(k, weight, weight_new, kind):
            buf = wrow if kind == 'rows' else wcol
            count = w // 256

            def part(ref, i):
                if kind == 'rows':
                    return ref.at[ds(i * 256, 256), :]
                return ref.at[:, ds(i * (512 if kind == 'groups' else 256), 256)]

            def load(i):
                return pltpu.make_async_copy(part(weight, i), buf.at[lax.rem(i, 3)], wl_sem.at[lax.rem(i, 3)])

            def store(i):
                return pltpu.make_async_copy(buf.at[lax.rem(i, 3)], part(weight_new, i), ws_sem.at[lax.rem(i, 3)])

            load(jnp.int32(0)).start()
            load(jnp.int32(1)).start()

            def one(i, carry):
                cols = ds(i * 256, 256)
                slot = lax.rem(i, 3)
                load(i).wait()

                def put(x_orth):
                    buf[slot] = weight_step(buf[slot], x_orth.T if kind == 'rows' else x_orth, scale)

                if phase == DOWN:
                    put(xbuf[:, cols].astype(F32))
                else:
                    @pl.when(core == k)
                    def _():
                        put(xbuf[:, cols].astype(F32))

                    @pl.when(core != k)
                    def _():
                        put(xr[:, cols])
                store(i).start()

                @pl.when(i >= 1)
                def _():
                    store(i - 1).wait()

                @pl.when(i + 2 < count)
                def _():
                    load(i + 2).start()
                return carry

            lax.fori_loop(0, count, one, 0)
            store(jnp.int32(count - 1)).wait()

        return weights

    load_grads(jnp.int32(0), 0, 0)
    load_grads(jnp.int32(1), 1, 1)
    services(0, 19)
    w_long, w_mid = w_gate.shape[1], w_o.shape[0]

    def scale_of(w):
        return 0.2 * math.sqrt(max(d, 2 * w))

    weights = newton(DOWN, w_long, scale_of(w_long), 20)
    weights(0, w_down, wn_down, 'rows')
    services(30, 43)
    weights = newton(GATE_UP, w_long, scale_of(w_long), 44)
    weights(0, w_gate, wn_gate, 'cols')
    service(jnp.int32(54), 54, 54)
    weights(1, w_up, wn_up, 'cols')
    services(55, 59)
    weights = newton(O_Q, w_mid, scale_of(w_mid), 60)
    weights(0, w_o, wn_o, 'rows')
    services(70, PAIRS + 7)
    weights(1, w_qkv, wn_qkv, 'groups')
    normalize(KEY_VALUE, 2 * GROUP_COLS, sb_ref)
    copy = pltpu.make_async_copy(sb_ref, kv_out, kv_sem)
    copy.start()
    for slot in range(4):
        for k in range(2):
            waited(mst.at[slot, k], ms_sem.at[slot, k])
    copy.wait()


def main_step(grads, weights, moms):
    any_spec = pl.BlockSpec(memory_space=pl.ANY)
    ins = list(grads) + list(weights) + list(moms)
    d, width = weights[0].shape
    outs = [jax.ShapeDtypeStruct(a.shape, F32) for a in list(weights) + list(moms)] + [jax.ShapeDtypeStruct((d, d), BF16)]
    w_long = weights[2].shape[1]
    dma = pltpu.SemaphoreType.DMA
    pieces = (PIECE_R, PIECE_C)
    return pl.pallas_call(
        step_kernel,
        out_shape=outs,
        in_specs=[any_spec] * len(ins),
        out_specs=[any_spec] * len(outs),
        scratch_shapes=[
            pltpu.VMEM((2, d, w_long), F32), pltpu.VMEM((d, 2 * w_long), BF16), pltpu.VMEM((d, d), F32), pltpu.VMEM((d, d), BF16),
            pltpu.VMEM((d, d), BF16), pltpu.VMEM((d, w_long), F32), pltpu.VMEM((3, 256, d), F32), pltpu.VMEM((3, d, 256), F32),
            pltpu.VMEM((4, 2, HALF_R, PIECE_C), F32), pltpu.VMEM((4, 2, HALF_R, PIECE_C), F32),
            pltpu.VMEM((8, 2, HALF_R, PIECE_C), F32), pltpu.VMEM((8, 2, QUART_R, PIECE_C), F32), pltpu.VMEM((8, 2) + pieces, F32),
            pltpu.VMEM((8, 2) + pieces, BF16), pltpu.VMEM((4, 2) + pieces, F32), pltpu.VMEM((4, 2) + pieces, F32),
            pltpu.VMEM((2,) + pieces, F32), pltpu.VMEM((2, PIECE_C, PIECE_R), F32),
            dma((8, 2)), dma((4, 2)), dma((4, 2)), dma((4, 2)), dma((4, 2)), dma((8, 2)), dma((8, 2)), dma((8, 2)),
            dma((8, 2)), dma((8, 2)), dma((8, 2)), dma((8, 2)), dma((8, 2)),
            dma((2,)), dma, dma((4,)), dma((2,)), dma((3,)), dma((3,)), dma((3,)), dma, pltpu.SemaphoreType.REGULAR],
        compiler_params=pltpu.CompilerParams(vmem_limit_bytes=VMEM_BYTES, collective_id=0, has_side_effects=True),
        cost_estimate=pl.CostEstimate(flops=10 ** 11, bytes_accessed=2 * 10 ** 8, transcendentals=0),
    )(*ins)


def update_other(weight, x_back, weight_new, scale, core):
    rows, width = x_back.shape
    theirs = pl.BlockSpec((rows, HEAD_DIM), lambda g, c: (0, 4 * g + 3 - c[0]))

    def body(c_ref, w_ref, back_ref, unused, o_ref):
        o_ref[...] = weight_step(w_ref[...], back_ref[...], scale)

    moved = 12 * rows * width
    return pl.pallas_call(
        body, out_shape=jax.ShapeDtypeStruct(weight.shape, F32),
        grid_spec=pltpu.PrefetchScalarGridSpec(
            num_scalar_prefetch=1, grid=(width // HEAD_DIM,),
            in_specs=[theirs, pl.BlockSpec((rows, HEAD_DIM), lambda g, c: (0, g)), pl.BlockSpec(memory_space=pl.ANY)],
            out_specs=theirs),
        input_output_aliases={3: 0},
        compiler_params=pltpu.CompilerParams(vmem_limit_bytes=VMEM_BYTES),
        cost_estimate=pl.CostEstimate(flops=moved, bytes_accessed=moved, transcendentals=0),
    )(core, weight, x_back, weight_new)


PARTS = 4


def finish_kernel(*refs):
    x_in, w_qkv = refs[:2]
    srcs, out_far, dsts = refs[2:12], refs[12], refs[13:23]
    x_ref, s_ref, sb_ref, t_ref, wk = refs[23:28]
    bufs = refs[28:38]
    in_sem, out_sem, wl_sem, ws_sem, x_sem = refs[38:]
    d, w = out_far.shape
    load = pltpu.make_async_copy(x_in, x_ref, x_sem)
    load.start()
    core = lax.axis_index('tp')
    heads = [(g * HEAD_DIM, ds((4 * g + 2 + core) * HEAD_DIM, HEAD_DIM)) for g in range(w // HEAD_DIM)]
    scale = 0.2 * math.sqrt(max(d, 2 * w))
    for lo, at in heads:
        pltpu.make_async_copy(w_qkv.at[:, at], wk.at[:, lo:lo + HEAD_DIM], wl_sem).start()

    def fetch(n, i):
        rows = srcs[n].shape[0] // PARTS
        return pltpu.make_async_copy(srcs[n].at[ds(i * rows, rows), :], bufs[n], in_sem.at[n])

    def put(n, i):
        rows = srcs[n].shape[0] // PARTS
        return pltpu.make_async_copy(bufs[n], dsts[n].at[ds(i * rows, rows), :], out_sem.at[n])

    def fetch_at(n, i):
        i = i - n // 5

        @pl.when((i > 0) & (i < PARTS))
        def _():
            put(n, i - 1).wait()

        @pl.when((i >= 0) & (i < PARTS))
        def _():
            fetch(n, i).start()

    def put_at(n, i):
        i = i - n // 5

        @pl.when((i >= 0) & (i < PARTS))
        def _():
            fetch(n, i).wait()
            put(n, i).start()

    def step(i, carry):
        starts = {0: (0, 5), 2: (1, 6), 4: (2, 7), 6: (3, 8), 8: (4, 9)}
        ends = {3: (0, 5), 5: (1, 6), 7: (2, 7)}
        slots = iter(range(9))

        def between():
            slot = next(slots)
            for n in ends.get(slot, ()):
                put_at(n, i)
            for n in starts.get(slot, ()):
                fetch_at(n, i)

        between()
        gram_step(x_ref, 2 * w, s_ref, sb_ref, between)
        poly_step(s_ref, sb_ref, t_ref, between)

        @pl.when(i < NEWTON_STEPS - 1)
        def _():
            def move(c, inner):
                cols = ds(c * PANEL, PANEL)
                x_ref[:, cols] = advanced(t_ref, x_ref, cols)
                return inner
            lax.fori_loop(0, 2 * w // PANEL, move, 0)
        for n in (3, 8, 4, 9):
            put_at(n, i)
        return carry

    load.wait()
    lax.fori_loop(0, NEWTON_STEPS, step, 0)
    for c in range(w // PANEL):
        cols = slice(c * PANEL, (c + 1) * PANEL)
        out_far[:, cols] = advanced(t_ref, x_ref, pl.ds(w + c * PANEL, PANEL)).astype(F32)
    pltpu.make_async_copy(wk, wk, wl_sem).wait()
    for c in range(w // PANEL):
        cols = slice(c * PANEL, (c + 1) * PANEL)
        wk[:, cols] = weight_step(wk[:, cols], advanced(t_ref, x_ref, pl.ds(c * PANEL, PANEL)).astype(F32), scale)
    for n in range(10):
        put(n, PARTS - 1).wait()
    for lo, at in heads:
        pltpu.make_async_copy(wk.at[:, lo:lo + HEAD_DIM], dsts[0].at[:, at], ws_sem).start()
    pltpu.make_async_copy(wk, wk, ws_sem).wait()


def finish(x_kv, w_qkv, arrays):
    d = x_kv.shape[0]
    w = x_kv.shape[1] // 2
    any_spec = pl.BlockSpec(memory_space=pl.ANY)
    vmem = pl.BlockSpec(memory_space=pltpu.VMEM)
    dma = pltpu.SemaphoreType.DMA
    return pl.pallas_call(
        finish_kernel,
        out_shape=[jax.ShapeDtypeStruct((d, w), F32)] + [jax.ShapeDtypeStruct(a.shape, F32) for a in arrays],
        in_specs=[any_spec] * (len(arrays) + 2),
        out_specs=[vmem] + [any_spec] * len(arrays),
        scratch_shapes=[pltpu.VMEM((d, d), BF16), pltpu.VMEM((d, d), F32), pltpu.VMEM((d, d), BF16), pltpu.VMEM((d, d), BF16), pltpu.VMEM((d, w), F32)]
        + [pltpu.VMEM((a.shape[0] // PARTS, a.shape[1]), F32) for a in arrays] + [dma((10,)), dma((10,)), dma, dma, dma],
        compiler_params=pltpu.CompilerParams(vmem_limit_bytes=VMEM_BYTES),
        cost_estimate=pl.CostEstimate(flops=3 * 10 ** 10, bytes_accessed=12 * 10 ** 7, transcendentals=0),
    )(x_kv, w_qkv, *arrays)


def solution(mesh):
    tp_count = mesh.shape['tp']
    col_spec = P(None, 'tp')
    row_spec = P('tp', None)
    grad_col = P('dp', None, 'tp')
    grad_row = P('dp', 'tp', None)
    weight_specs = (col_spec, row_spec, col_spec, col_spec, row_spec)
    in_specs = (grad_col, grad_row, grad_col, grad_col, grad_row) + weight_specs + weight_specs
    out_specs = weight_specs + weight_specs
    swap = [(0, 1), (1, 0)]

    def local_step(*arrays):
        weights, moms = arrays[5:10], arrays[10:]
        results = main_step([block[0] for block in arrays[:5]], weights, moms)
        done = finish(results[10], weights[0], results[:10])
        x_far, done = done[0], list(done[1:])
        scale = 0.2 * math.sqrt(max(x_far.shape[0], x_far.shape[1] * tp_count))
        core = lax.axis_index('tp').astype(jnp.int32).reshape(1)
        done[0] = update_other(weights[0], lax.ppermute(x_far, 'tp', swap), done[0], scale, core)
        return tuple(done)

    return jax.shard_map(local_step, mesh=mesh, in_specs=in_specs, out_specs=out_specs, check_vma=False)
```

```python
import functools
import math
import jax
import jax.numpy as jnp
from jax import lax
from jax.experimental import pallas as pl
from jax.experimental.pallas import tpu as pltpu
from jax.sharding import PartitionSpec as P

HEAD_DIM = 128
NEWTON_STEPS = 5
COEFF_A = 3.4445
COEFF_B = -4.7750
COEFF_C = 2.0315
MOMENTUM = 0.95
LEARN_RATE = 2e-3
WEIGHT_DECAY = 0.1
EPSILON = 1e-7
PANEL = 512
VMEM_BYTES = 67043328
F32 = jnp.float32
BF16 = jnp.bfloat16


GROUP_COLS = 2 * HEAD_DIM
MESH = pl.DeviceIdType.MESH
PIECE_R = 128
PIECE_C = 512
HALF_R = PIECE_R // 2
QUART_R = PIECE_R // 4
DOWN, GATE_UP, O_Q, KEY_VALUE = range(4)
KV_DELAY = 5
FIRST = (0, 12, 36, 52 + KV_DELAY)
LAST = (12, 36, 52, 60 + KV_DELAY)
PAIRS = LAST[-1]
BLOCK = 512


def ds(start, size):
    return pl.ds(start if isinstance(start, int) else pl.multiple_of(start, math.gcd(size, 128)), size)


def moved_momentum(grad, mom):
    mom_new = MOMENTUM * mom + grad
    return mom_new, grad + MOMENTUM * mom_new


def weight_step(weight, x_orth, scale):
    return weight - LEARN_RATE * (scale * x_orth + WEIGHT_DECAY * weight)


def gram_panel(x_ref, depth, j, block):
    return lax.dot_general(x_ref[:(j + 1) * block, :depth], x_ref[j * block:(j + 1) * block, :depth], (((1,), (1,)), ((), ())),
                           preferred_element_type=F32)


def gram_step(x_ref, depth, s_ref, sb_ref, block):
    for j in range(s_ref.shape[0] // block):
        cols = slice(j * block, (j + 1) * block)
        part = gram_panel(x_ref, depth, j, block)
        s_ref[:(j + 1) * block, cols] = part
        half = part.astype(BF16)
        sb_ref[:(j + 1) * block, cols] = half
        if j:
            sb_ref[cols, :j * block] = half[:j * block, :].T


def poly_step(s_ref, sb_ref, t_ref, block):
    for j in range(s_ref.shape[0] // block):
        cols = slice(j * block, (j + 1) * block)
        part = jnp.dot(sb_ref[:(j + 1) * block, :], sb_ref[:, cols], preferred_element_type=F32)
        poly_part = (COEFF_B * s_ref[:(j + 1) * block, cols] + COEFF_C * part).astype(BF16)
        t_ref[:(j + 1) * block, cols] = poly_part
        if j:
            t_ref[cols, :j * block] = poly_part[:j * block, :].T


def advanced(t_ref, x_ref, cols):
    x_cur = x_ref[:, cols]
    prod = jnp.dot(t_ref[...], x_cur, preferred_element_type=F32)
    return (COEFF_A * x_cur.astype(F32) + prod).astype(BF16)


def step_kernel(*refs):
    (g_qkv, g_o, g_gate, g_up, g_down, w_qkv, w_o, w_gate, w_up, w_down, m_qkv, m_o, m_gate, m_up, m_down,
     wn_qkv, wn_o, wn_gate, wn_up, wn_down, mn_qkv, mn_o, mn_gate, mn_up, mn_down, kv_out,
     nbuf, xbuf, s_ref, sb_ref, t_ref, xr, wrow, wcol, snd1, half, r1, r2, fin, gbuf, mbuf, mst, nst, nst_t,
     g_sem, m_sem, ms_sem, send1, send2, send3, send4, send5, recv1, recv2, recv3, recv4, recv5,
     nsend, dsend, nrecv, xsend, xrecv, wl_sem, ws_sem, kv_sem, credit) = refs
    dp = lax.axis_index('dp')
    core = lax.axis_index('tp')
    far = 1 - core
    pos_y, pos_x = lax.div(dp, 2), lax.rem(dp, 2)
    across = (pos_y * 2 + 1 - pos_x, (1 - pos_y) * 2 + pos_x)
    place = ((pos_x, pos_y), (pos_y, pos_x))
    d = s_ref.shape[0]

    def toward(k, second):
        return {'dp': across[k ^ second]}

    barrier = pltpu.get_barrier_semaphore()
    for where in ({'dp': across[0]}, {'dp': across[1]}, {'tp': far}):
        pl.semaphore_signal(barrier, inc=1, device_id=where, device_id_type=MESH)
    pl.semaphore_wait(barrier, 3)

    def blocks(phase, k, t, mats):
        j = t - FIRST[phase]
        qkv, o, gate, up, down = mats
        if phase == DOWN:
            return [(down.at[ds(j * PIECE_R, PIECE_R), pl.ds(k * PIECE_C, PIECE_C)], slice(0, PIECE_C))]
        if phase == GATE_UP:
            return [((gate, up)[k].at[ds(lax.div(j, 3) * PIECE_R, PIECE_R), ds(lax.rem(j, 3) * PIECE_C, PIECE_C)], slice(0, PIECE_C))]
        if phase == O_Q and k == 0:
            return [(o.at[ds(lax.div(j, 2) * PIECE_R, PIECE_R), ds(lax.rem(j, 2) * PIECE_C, PIECE_C)], slice(0, PIECE_C))]
        row, part, skip = (lax.div(j, 2), lax.rem(j, 2), 0) if phase == O_Q else (j, k, GROUP_COLS)
        return [(qkv.at[ds(row * PIECE_R, PIECE_R), ds(part * 4 * GROUP_COLS + skip + 2 * g * GROUP_COLS, GROUP_COLS)],
                 slice(g * GROUP_COLS, (g + 1) * GROUP_COLS)) for g in range(2)]

    def by_phase(t, low, high, phases, fn):
        for phase in phases:
            first, last = FIRST[phase], LAST[phase]
            if high < first or low >= last:
                continue
            if low >= first and high < last:
                fn(phase)
            else:
                pl.when((t >= first) & (t < last))(functools.partial(fn, phase))

    grads = (g_qkv, g_o, g_gate, g_up, g_down)
    moms = (m_qkv, m_o, m_gate, m_up, m_down)
    mom_news = (mn_qkv, mn_o, mn_gate, mn_up, mn_down)

    def waited(ref, sem):
        pltpu.make_async_copy(ref, ref, sem).wait()

    def load_grads(t, low, high):
        def start(phase):
            for k in range(2):
                for ref, cols in blocks(phase, k, t, grads):
                    pltpu.make_async_copy(ref, gbuf.at[lax.rem(t, 8), k, :, cols], g_sem.at[lax.rem(t, 8), k]).start()
        by_phase(t, low, high, range(4), start)

    def remote(src, dst, send, recv, where):
        return pltpu.make_async_remote_copy(src_ref=src, dst_ref=dst, send_sem=send, recv_sem=recv, device_id=where,
                                            device_id_type=MESH)

    def copies(k, t, which):
        s4, s8 = lax.rem(t, 4), lax.rem(t, 8)
        a, b = place[k]
        keep = ds(a * HALF_R + b * QUART_R, QUART_R)
        got = ds(a * HALF_R + (1 - b) * QUART_R, QUART_R)
        if which == 0:
            return remote(snd1.at[s4, k], r1.at[s8, k], send1.at[s4, k], recv1.at[s8, k], toward(k, 0))
        if which == 1:
            return remote(half.at[s4, k, ds((1 - b) * QUART_R, QUART_R)], r2.at[s8, k], send2.at[s4, k], recv2.at[s8, k], toward(k, 1))
        if which == 2:
            return remote(fin.at[s8, k, keep], fin.at[s8, k, keep], send3.at[s8, k], recv3.at[s8, k], toward(k, 1))
        if which == 3:
            return remote(fin.at[s8, k, keep], fin.at[s8, k, keep], send4.at[s8, k], recv4.at[s8, k], toward(k, 0))
        return remote(fin.at[s8, k, got], fin.at[s8, k, got], send5.at[s8, k], recv5.at[s8, k], toward(k, 0))

    def send_half(t, low, high):
        s4, s8 = lax.rem(t, 4), lax.rem(t, 8)
        for k in range(2):
            waited(gbuf.at[s8, k], g_sem.at[s8, k])
            a = place[k][0]
            snd1[s4, k] = gbuf[s8, k, ds((1 - a) * HALF_R, HALF_R), :].astype(F32)
            copies(k, t, 0).start()

    def send_quarter(t, low, high):
        s4, s8 = lax.rem(t, 4), lax.rem(t, 8)
        for k in range(2):
            copies(k, t, 0).wait()
            a = place[k][0]
            half[s4, k] = gbuf[s8, k, ds(a * HALF_R, HALF_R), :].astype(F32) + r1[s8, k]
            copies(k, t, 1).start()

    def share_quarter(t, low, high):
        s4, s8 = lax.rem(t, 4), lax.rem(t, 8)
        for k in range(2):
            copies(k, t, 1).wait()
            a, b = place[k]
            fin[s8, k, ds(a * HALF_R + b * QUART_R, QUART_R), :] = (half[s4, k, ds(b * QUART_R, QUART_R), :] + r2[s8, k]) * 0.25
            copies(k, t, 2).start()
            copies(k, t, 3).start()

    def pass_quarter(t, low, high):
        s4 = lax.rem(t, 4)
        for k in range(2):
            copies(k, t, 2).wait_recv()
            copies(k, t, 4).start()

        def start(phase):
            for k in range(2):
                for ref, cols in blocks(phase, k, t, moms):
                    pltpu.make_async_copy(ref, mbuf.at[s4, k, :, cols], m_sem.at[s4, k]).start()
        by_phase(t, low, high, range(4), start)

    def away_block(t, phase, k):
        j = t - FIRST[phase]
        s2 = lax.rem(t, 2)
        if phase == GATE_UP:
            src, rows, cols = nst.at[s2], ds(lax.div(j, 3) * PIECE_R, PIECE_R), ds(lax.rem(j, 3) * PIECE_C, PIECE_C)
        elif k == 0:
            src, rows, cols = nst_t.at[s2], ds(lax.rem(j, 2) * PIECE_C, PIECE_C), ds(lax.div(j, 2) * PIECE_R, PIECE_R)
        else:
            src, rows, cols = nst.at[s2], ds(lax.div(j, 2) * PIECE_R, PIECE_R), ds(lax.rem(j, 2) * PIECE_C, PIECE_C)
        return src, rows, cols

    def retire(t, low, high):
        s2, s4, s8 = lax.rem(t, 2), lax.rem(t, 4), lax.rem(t, 8)
        for k in range(2):
            copies(k, t, 2).wait_send()
            copies(k, t, 3).wait()
            copies(k, t, 4).wait()

        def finish(phase):
            if phase:
                @pl.when(t == FIRST[phase])
                def _():
                    pl.semaphore_wait(credit, 1)

                @pl.when(t > FIRST[phase])
                def _():
                    waited(nst.at[lax.rem(t + 1, 2)], nsend.at[lax.rem(t + 1, 2)])
            for k in range(2):
                waited(mbuf.at[s4, k], m_sem.at[s4, k])
                if phase:
                    waited(mst.at[s4, k], ms_sem.at[s4, k])
                else:
                    @pl.when(t >= 4)
                    def _():
                        waited(mst.at[s4, k], ms_sem.at[s4, k])
                mom_new, nest = moved_momentum(fin[s8, k], mbuf[s4, k])
                mst[s4, k] = mom_new
                for ref, cols in blocks(phase, k, t, mom_news):
                    pltpu.make_async_copy(mst.at[s4, k, :, cols], ref, ms_sem.at[s4, k]).start()
                if phase == DOWN:
                    rows, cols = pl.ds(k * PIECE_C, PIECE_C), ds(t * PIECE_R, PIECE_R)
                    nbuf[core, rows, cols] = nest.T
                    remote(nbuf.at[core, rows, cols], nbuf.at[core, rows, cols], dsend, nrecv.at[DOWN], {'tp': far}).start()
                    continue
                if phase == KEY_VALUE:
                    rows = ds((t - FIRST[KEY_VALUE]) * PIECE_R, PIECE_R)

                    def split(mine, nest=nest, k=k):
                        for g in range(2):
                            cols = slice((2 * k + g) * HEAD_DIM, (2 * k + g + 1) * HEAD_DIM)
                            heads = [nest[:, (2 * g + h) * HEAD_DIM:(2 * g + h + 1) * HEAD_DIM] for h in range(2)]
                            nbuf[core, rows, cols] = heads[mine]
                            nst[s2, :, cols] = heads[1 - mine]
                    pl.when(core == 0)(functools.partial(split, 0))
                    pl.when(core == 1)(functools.partial(split, 1))
                    if k:
                        remote(nst.at[s2], nbuf.at[core, rows, pl.ds(0, 2 * GROUP_COLS)], nsend.at[s2], nrecv.at[phase], {'tp': far}).start()
                    continue
                turned = phase == O_Q and k == 0
                piece = nest.T if turned else nest
                src, rows, cols = away_block(t, phase, k)

                @pl.when(core == k)
                def _():
                    nbuf[core, rows, cols] = piece

                @pl.when(core != k)
                def _():
                    (nst_t if turned else nst)[s2] = piece
                    remote(src, nbuf.at[core, rows, cols], nsend.at[s2], nrecv.at[phase], {'tp': far}).start()
        by_phase(t, low, high, range(4), finish)

    def service(s, low, high):
        for offset, stage in ((6, pass_quarter), (4, share_quarter), (2, send_quarter), (0, send_half), (8, retire), (-2, load_grads)):
            t, lo, hi = s - offset, low - offset, high - offset
            if hi < 0 or lo >= PAIRS:
                continue
            run = functools.partial(stage, t, max(lo, 0), min(hi, PAIRS - 1))
            guards = []
            if lo < 0:
                guards.append(t >= 0)
            if hi >= PAIRS:
                guards.append(t < PAIRS)
            if KV_DELAY and lo < FIRST[KEY_VALUE] and hi >= LAST[O_Q]:
                if lo >= LAST[O_Q] and hi < FIRST[KEY_VALUE]:
                    continue
                guards.append((t - LAST[O_Q]) * (t - FIRST[KEY_VALUE] + 1) > 0)
            if guards:
                pl.when(functools.reduce(jnp.logical_and, guards))(run)
            else:
                run()

    def services(low, high):
        def one(s, carry):
            service(s, low, high)
            return carry
        lax.fori_loop(low, high + 1, one, 0)

    def normalize(phase, w, x_out):
        waited(nbuf.at[far, :, pl.ds(0, w)], nrecv.at[phase])
        if phase == DOWN:
            waited(nbuf.at[core, :, pl.ds(0, w)], dsend)
        else:
            end = (LAST[phase] - 1) % 2
            waited(nst.at[end], nsend.at[end])
        rows_step = 64

        def square_rows(r, acc):
            rows = ds(r * rows_step, rows_step)
            a = nbuf[core, rows, :w]
            b = nbuf[far, rows, :w]
            return acc + (a * a + b * b)

        acc = lax.fori_loop(0, d // rows_step, square_rows, jnp.zeros((rows_step, w), F32))
        inv = 1.0 / (jnp.sqrt(jnp.sum(acc)) + EPSILON)

        def fill_rows(r, carry):
            rows = ds(r * rows_step, rows_step)
            x_out[rows, :w] = (nbuf[core, rows, :w] * inv).astype(BF16)
            x_out[rows, w:2 * w] = (nbuf[far, rows, :w] * inv).astype(BF16)
            return carry

        lax.fori_loop(0, d // rows_step, fill_rows, 0)

    def newton(phase, w, scale, first_service):
        normalize(phase, w, xbuf)
        pl.semaphore_signal(credit, inc=1, device_id={'tp': far}, device_id_type=MESH)

        def step(i, carry):
            block = BLOCK if phase == O_Q else PANEL
            gram_step(xbuf, 2 * w, s_ref, sb_ref, block)
            last = first_service + 2 * NEWTON_STEPS - 1
            service(first_service + 2 * i, first_service, last)
            poly_step(s_ref, sb_ref, t_ref, block)

            @pl.when(i < NEWTON_STEPS - 1)
            def _():
                def move(c, inner):
                    cols = ds(c * PANEL, PANEL)
                    xbuf[:, cols] = advanced(t_ref, xbuf, cols)
                    return inner
                lax.fori_loop(0, 2 * w // PANEL, move, 0)
            service(first_service + 2 * i + 1, first_service, last)
            return carry

        lax.fori_loop(0, NEWTON_STEPS, step, 0)
        count = w // PANEL
        if phase != DOWN:
            def return_copy(c):
                cols = slice((c % 2) * PANEL, (c % 2 + 1) * PANEL)
                return remote(s_ref.at[:, cols], xr.at[:, pl.ds(c * PANEL, PANEL)], xsend.at[c % 2], xrecv.at[phase], {'tp': far})

            for c in range(count):
                if c >= 2:
                    return_copy(c - 2).wait_send()
                s_ref[:, (c % 2) * PANEL:(c % 2 + 1) * PANEL] = advanced(t_ref, xbuf, pl.ds(w + c * PANEL, PANEL)).astype(F32)
                return_copy(c).start()

        def own(c, carry):
            cols = ds(c * PANEL, PANEL)
            xbuf[:, cols] = advanced(t_ref, xbuf, cols)
            return carry

        lax.fori_loop(0, count, own, 0)
        if phase != DOWN:
            for c in range(max(count - 2, 0), count):
                return_copy(c).wait_send()
            waited(xr.at[:, pl.ds(0, w)], xrecv.at[phase])

        def weights(k, weight, weight_new, kind, first=None):
            buf = wrow if kind == 'rows' else wcol
            count = w // 256

            def part(ref, i):
                if kind == 'rows':
                    return ref.at[ds(i * 256, 256), :]
                return ref.at[:, ds(i * (512 if kind == 'groups' else 256), 256)]

            def load(i):
                return pltpu.make_async_copy(part(weight, i), buf.at[lax.rem(i, 3)], wl_sem.at[lax.rem(i, 3)])

            def store(i):
                return pltpu.make_async_copy(buf.at[lax.rem(i, 3)], part(weight_new, i), ws_sem.at[lax.rem(i, 3)])

            load(jnp.int32(0)).start()
            load(jnp.int32(1)).start()

            def one(i, carry):
                cols = ds(i * 256, 256)
                slot = lax.rem(i, 3)
                load(i).wait()

                def put(x_orth):
                    buf[slot] = weight_step(buf[slot], x_orth.T if kind == 'rows' else x_orth, scale)

                if phase == DOWN:
                    put(xbuf[:, cols].astype(F32))
                else:
                    @pl.when(core == k)
                    def _():
                        put(xbuf[:, cols].astype(F32))

                    @pl.when(core != k)
                    def _():
                        put(xr[:, cols])
                store(i).start()

                @pl.when(i >= 1)
                def _():
                    store(i - 1).wait()

                @pl.when(i + 2 < count)
                def _():
                    load(i + 2).start()
                if first is not None:
                    @pl.when(lax.rem(i, 3) == 2)
                    def _():
                        service(first + lax.div(i, 3), first, first + 1)
                return carry

            lax.fori_loop(0, count, one, 0)
            store(jnp.int32(count - 1)).wait()

        return weights

    load_grads(jnp.int32(0), 0, 0)
    load_grads(jnp.int32(1), 1, 1)
    services(0, 19)
    w_long, w_mid = w_gate.shape[1], w_o.shape[0]

    def scale_of(w):
        return 0.2 * math.sqrt(max(d, 2 * w))

    weights = newton(DOWN, w_long, scale_of(w_long), 20)
    weights(0, w_down, wn_down, 'rows', 30)
    services(32, 43)
    weights = newton(GATE_UP, w_long, scale_of(w_long), 44)
    weights(0, w_gate, wn_gate, 'cols', 54)
    weights(1, w_up, wn_up, 'cols')
    services(56, 59)
    weights = newton(O_Q, w_mid, scale_of(w_mid), 60)
    weights(0, w_o, wn_o, 'rows')
    services(70, PAIRS + 7)
    weights(1, w_qkv, wn_qkv, 'groups')
    normalize(KEY_VALUE, 2 * GROUP_COLS, sb_ref)
    copy = pltpu.make_async_copy(sb_ref, kv_out, kv_sem)
    copy.start()
    for slot in range(4):
        for k in range(2):
            waited(mst.at[slot, k], ms_sem.at[slot, k])
    copy.wait()


def main_step(grads, weights, moms):
    any_spec = pl.BlockSpec(memory_space=pl.ANY)
    ins = list(grads) + list(weights) + list(moms)
    d, width = weights[0].shape
    outs = [jax.ShapeDtypeStruct(a.shape, F32) for a in list(weights) + list(moms)] + [jax.ShapeDtypeStruct((d, d), BF16)]
    w_long = weights[2].shape[1]
    dma = pltpu.SemaphoreType.DMA
    pieces = (PIECE_R, PIECE_C)
    return pl.pallas_call(
        step_kernel,
        out_shape=outs,
        in_specs=[any_spec] * len(ins),
        out_specs=[any_spec] * len(outs),
        scratch_shapes=[
            pltpu.VMEM((2, d, w_long), F32), pltpu.VMEM((d, 2 * w_long), BF16), pltpu.VMEM((d, d), F32), pltpu.VMEM((d, d), BF16),
            pltpu.VMEM((d, d), BF16), pltpu.VMEM((d, w_long), F32), pltpu.VMEM((3, 256, d), F32), pltpu.VMEM((3, d, 256), F32),
            pltpu.VMEM((4, 2, HALF_R, PIECE_C), F32), pltpu.VMEM((4, 2, HALF_R, PIECE_C), F32),
            pltpu.VMEM((8, 2, HALF_R, PIECE_C), F32), pltpu.VMEM((8, 2, QUART_R, PIECE_C), F32), pltpu.VMEM((8, 2) + pieces, F32),
            pltpu.VMEM((8, 2) + pieces, BF16), pltpu.VMEM((4, 2) + pieces, F32), pltpu.VMEM((4, 2) + pieces, F32),
            pltpu.VMEM((2,) + pieces, F32), pltpu.VMEM((2, PIECE_C, PIECE_R), F32),
            dma((8, 2)), dma((4, 2)), dma((4, 2)), dma((4, 2)), dma((4, 2)), dma((8, 2)), dma((8, 2)), dma((8, 2)),
            dma((8, 2)), dma((8, 2)), dma((8, 2)), dma((8, 2)), dma((8, 2)),
            dma((2,)), dma, dma((4,)), dma((2,)), dma((3,)), dma((3,)), dma((3,)), dma, pltpu.SemaphoreType.REGULAR],
        compiler_params=pltpu.CompilerParams(vmem_limit_bytes=VMEM_BYTES, collective_id=0, has_side_effects=True),
        cost_estimate=pl.CostEstimate(flops=10 ** 11, bytes_accessed=2 * 10 ** 8, transcendentals=0),
    )(*ins)


def update_other(weight, x_back, weight_new, scale, core):
    rows, width = x_back.shape
    theirs = pl.BlockSpec((rows, HEAD_DIM), lambda g, c: (0, 4 * g + 3 - c[0]))

    def body(c_ref, w_ref, back_ref, unused, o_ref):
        o_ref[...] = weight_step(w_ref[...], back_ref[...], scale)

    moved = 12 * rows * width
    return pl.pallas_call(
        body, out_shape=jax.ShapeDtypeStruct(weight.shape, F32),
        grid_spec=pltpu.PrefetchScalarGridSpec(
            num_scalar_prefetch=1, grid=(width // HEAD_DIM,),
            in_specs=[theirs, pl.BlockSpec((rows, HEAD_DIM), lambda g, c: (0, g)), pl.BlockSpec(memory_space=pl.ANY)],
            out_specs=theirs),
        input_output_aliases={3: 0},
        compiler_params=pltpu.CompilerParams(vmem_limit_bytes=VMEM_BYTES),
        cost_estimate=pl.CostEstimate(flops=moved, bytes_accessed=moved, transcendentals=0),
    )(core, weight, x_back, weight_new)


def finish_kernel(*refs):
    x_in, w_qkv = refs[:2]
    srcs, out_far, dsts = refs[2:12], refs[12], refs[13:23]
    x_ref, s_ref, sb_ref, t_ref, wk = refs[23:28]
    bufs = refs[28:34]
    in_sem, out_sem, wl_sem, ws_sem, x_sem = refs[34:]
    d, w = out_far.shape
    load = pltpu.make_async_copy(x_in, x_ref, x_sem)
    load.start()
    core = lax.axis_index('tp')
    heads = [(g * HEAD_DIM, ds((4 * g + 2 + core) * HEAD_DIM, HEAD_DIM)) for g in range(w // HEAD_DIM)]
    scale = 0.2 * math.sqrt(max(d, 2 * w))
    for lo, at in heads:
        pltpu.make_async_copy(w_qkv.at[:, at], wk.at[:, lo:lo + HEAD_DIM], wl_sem).start()

    moves = [(srcs[n], dsts[n]) for n in (4, 9, 2, 7, 3, 8)]
    moves += [(srcs[n], dsts[n]) for n in (1, 6)]
    moves += [(srcs[n].at[:, lo:lo + d], dsts[n].at[:, lo:lo + d]) for n in (0, 5) for lo in (0, d)]

    def held(n):
        return bufs[n] if n < 6 else bufs[n - 6].at[:d, :d]

    def fetch(n):
        if n >= 6:
            put_copy(n - 6).wait()
        pltpu.make_async_copy(moves[n][0], held(n), in_sem.at[n]).start()

    def put_copy(n):
        return pltpu.make_async_copy(held(n), moves[n][1], out_sem.at[n])

    def put(n):
        pltpu.make_async_copy(moves[n][0], held(n), in_sem.at[n]).wait()
        put_copy(n).start()

    for n in range(6):
        fetch(n)
    plan = {(0, 1): ((put, 0),), (0, 2): ((put, 1),), (1, 0): ((put, 2),), (1, 1): ((put, 3),), (1, 2): ((fetch, 6),),
            (2, 0): ((put, 4),), (2, 1): ((put, 5), (fetch, 7)), (2, 2): ((fetch, 8),), (3, 0): ((put, 6), (fetch, 9)),
            (3, 1): ((put, 7), (fetch, 10)), (3, 2): ((put, 8),), (4, 0): ((fetch, 11), (put, 9)), (4, 1): ((put, 10),)}

    def step(i, carry):
        def at(slot):
            for turn in range(NEWTON_STEPS):
                if (turn, slot) in plan:
                    @pl.when(i == turn)
                    def _(todo=plan[turn, slot]):
                        for act, n in todo:
                            act(n)

        at(0)
        gram_step(x_ref, 2 * w, s_ref, sb_ref, BLOCK)
        at(1)
        poly_step(s_ref, sb_ref, t_ref, BLOCK)
        at(2)

        @pl.when(i < NEWTON_STEPS - 1)
        def _():
            def move(c, inner):
                cols = ds(c * PANEL, PANEL)
                x_ref[:, cols] = advanced(t_ref, x_ref, cols)
                return inner
            lax.fori_loop(0, 2 * w // PANEL, move, 0)
        return carry

    load.wait()
    lax.fori_loop(0, NEWTON_STEPS, step, 0)
    put(11)
    for c in range(w // PANEL):
        cols = slice(c * PANEL, (c + 1) * PANEL)
        out_far[:, cols] = advanced(t_ref, x_ref, pl.ds(w + c * PANEL, PANEL)).astype(F32)
    pltpu.make_async_copy(wk, wk, wl_sem).wait()
    for c in range(w // PANEL):
        cols = slice(c * PANEL, (c + 1) * PANEL)
        wk[:, cols] = weight_step(wk[:, cols], advanced(t_ref, x_ref, pl.ds(c * PANEL, PANEL)).astype(F32), scale)
    for n in range(6, 12):
        put_copy(n).wait()
    for lo, at in heads:
        pltpu.make_async_copy(wk.at[:, lo:lo + HEAD_DIM], dsts[0].at[:, at], ws_sem).start()
    pltpu.make_async_copy(wk, wk, ws_sem).wait()


def finish(x_kv, w_qkv, arrays):
    d = x_kv.shape[0]
    w = x_kv.shape[1] // 2
    any_spec = pl.BlockSpec(memory_space=pl.ANY)
    vmem = pl.BlockSpec(memory_space=pltpu.VMEM)
    dma = pltpu.SemaphoreType.DMA
    return pl.pallas_call(
        finish_kernel,
        out_shape=[jax.ShapeDtypeStruct((d, w), F32)] + [jax.ShapeDtypeStruct(a.shape, F32) for a in arrays],
        in_specs=[any_spec] * (len(arrays) + 2),
        out_specs=[vmem] + [any_spec] * len(arrays),
        scratch_shapes=[pltpu.VMEM((d, d), BF16), pltpu.VMEM((d, d), F32), pltpu.VMEM((d, d), BF16), pltpu.VMEM((d, d), BF16), pltpu.VMEM((d, w), F32)]
        + [pltpu.VMEM(arrays[n].shape, F32) for n in (4, 9, 2, 7, 3, 8)] + [dma((12,)), dma((12,)), dma, dma, dma],
        compiler_params=pltpu.CompilerParams(vmem_limit_bytes=VMEM_BYTES),
        cost_estimate=pl.CostEstimate(flops=3 * 10 ** 10, bytes_accessed=12 * 10 ** 7, transcendentals=0),
    )(x_kv, w_qkv, *arrays)


def solution(mesh):
    tp_count = mesh.shape['tp']
    col_spec = P(None, 'tp')
    row_spec = P('tp', None)
    grad_col = P('dp', None, 'tp')
    grad_row = P('dp', 'tp', None)
    weight_specs = (col_spec, row_spec, col_spec, col_spec, row_spec)
    in_specs = (grad_col, grad_row, grad_col, grad_col, grad_row) + weight_specs + weight_specs
    out_specs = weight_specs + weight_specs
    swap = [(0, 1), (1, 0)]

    def local_step(*arrays):
        weights, moms = arrays[5:10], arrays[10:]
        results = main_step([block[0] for block in arrays[:5]], weights, moms)
        done = finish(results[10], weights[0], results[:10])
        x_far, done = done[0], list(done[1:])
        scale = 0.2 * math.sqrt(max(x_far.shape[0], x_far.shape[1] * tp_count))
        core = lax.axis_index('tp').astype(jnp.int32).reshape(1)
        done[0] = update_other(weights[0], lax.ppermute(x_far, 'tp', swap), done[0], scale, core)
        return tuple(done)

    return jax.shard_map(local_step, mesh=mesh, in_specs=in_specs, out_specs=out_specs, check_vma=False)
```

```python
import functools
import math
import jax
import jax.numpy as jnp
from jax import lax
from jax.experimental import pallas as pl
from jax.experimental.pallas import tpu as pltpu
from jax.sharding import PartitionSpec as P

HEAD_DIM = 128
NEWTON_STEPS = 5
COEFF_A = 3.4445
COEFF_B = -4.7750
COEFF_C = 2.0315
MOMENTUM = 0.95
LEARN_RATE = 2e-3
WEIGHT_DECAY = 0.1
EPSILON = 1e-7
PANEL = 512
VMEM_BYTES = 67043328
F32 = jnp.float32
BF16 = jnp.bfloat16


GROUP_COLS = 2 * HEAD_DIM
MESH = pl.DeviceIdType.MESH
PIECE_R = 128
PIECE_C = 512
HALF_R = PIECE_R // 2
QUART_R = PIECE_R // 4
DOWN, GATE_UP, O_Q, KEY_VALUE = range(4)
KV_DELAY = 5
FIRST = (0, 12, 36, 52 + KV_DELAY)
LAST = (12, 36, 52, 60 + KV_DELAY)
PAIRS = LAST[-1]
BLOCK = 512


def ds(start, size):
    return pl.ds(start if isinstance(start, int) else pl.multiple_of(start, math.gcd(size, 128)), size)


def moved_momentum(grad, mom):
    mom_new = MOMENTUM * mom + grad
    return mom_new, grad + MOMENTUM * mom_new


def weight_step(weight, x_orth, scale):
    return weight - LEARN_RATE * (scale * x_orth + WEIGHT_DECAY * weight)


def gram_panel(x_ref, depth, j, block):
    return lax.dot_general(x_ref[:(j + 1) * block, :depth], x_ref[j * block:(j + 1) * block, :depth], (((1,), (1,)), ((), ())),
                           preferred_element_type=F32)


def gram_step(x_ref, depth, s_ref, sb_ref, block):
    for j in range(s_ref.shape[0] // block):
        cols = slice(j * block, (j + 1) * block)
        part = gram_panel(x_ref, depth, j, block)
        s_ref[:(j + 1) * block, cols] = part
        half = part.astype(BF16)
        sb_ref[:(j + 1) * block, cols] = half
        if j:
            sb_ref[cols, :j * block] = half[:j * block, :].T


def poly_step(s_ref, sb_ref, t_ref, block):
    for j in range(s_ref.shape[0] // block):
        cols = slice(j * block, (j + 1) * block)
        part = jnp.dot(sb_ref[:(j + 1) * block, :], sb_ref[:, cols], preferred_element_type=F32)
        poly_part = (COEFF_B * s_ref[:(j + 1) * block, cols] + COEFF_C * part).astype(BF16)
        t_ref[:(j + 1) * block, cols] = poly_part
        if j:
            t_ref[cols, :j * block] = poly_part[:j * block, :].T


def advanced(t_ref, x_ref, cols):
    x_cur = x_ref[:, cols]
    prod = jnp.dot(t_ref[...], x_cur, preferred_element_type=F32)
    return (COEFF_A * x_cur.astype(F32) + prod).astype(BF16)


def step_kernel(*refs):
    (g_qkv, g_o, g_gate, g_up, g_down, w_qkv, w_o, w_gate, w_up, w_down, m_qkv, m_o, m_gate, m_up, m_down,
     wn_gate, wn_up, wn_down, mn_qkv, mn_o, mn_gate, mn_up, mn_down, kv_out, own_out, other_out,
     nbuf, xbuf, s_ref, sb_ref, t_ref, xr, wrow, wcol, snd1, half, r1, r2, fin, gbuf, mbuf, mst, nst, nst_t,
     g_sem, m_sem, ms_sem, send1, send2, send3, send4, send5, recv1, recv2, recv3, recv4, recv5,
     nsend, dsend, nrecv, xsend, xrecv, wl_sem, ws_sem, kv_sem, credit) = refs
    dp = lax.axis_index('dp')
    core = lax.axis_index('tp')
    far = 1 - core
    pos_y, pos_x = lax.div(dp, 2), lax.rem(dp, 2)
    across = (pos_y * 2 + 1 - pos_x, (1 - pos_y) * 2 + pos_x)
    place = ((pos_x, pos_y), (pos_y, pos_x))
    d = s_ref.shape[0]

    def toward(k, second):
        return {'dp': across[k ^ second]}

    barrier = pltpu.get_barrier_semaphore()
    for where in ({'dp': across[0]}, {'dp': across[1]}, {'tp': far}):
        pl.semaphore_signal(barrier, inc=1, device_id=where, device_id_type=MESH)
    pl.semaphore_wait(barrier, 3)

    def blocks(phase, k, t, mats):
        j = t - FIRST[phase]
        qkv, o, gate, up, down = mats
        if phase == DOWN:
            return [(down.at[ds(j * PIECE_R, PIECE_R), pl.ds(k * PIECE_C, PIECE_C)], slice(0, PIECE_C))]
        if phase == GATE_UP:
            return [((gate, up)[k].at[ds(lax.div(j, 3) * PIECE_R, PIECE_R), ds(lax.rem(j, 3) * PIECE_C, PIECE_C)], slice(0, PIECE_C))]
        if phase == O_Q and k == 0:
            return [(o.at[ds(lax.div(j, 2) * PIECE_R, PIECE_R), ds(lax.rem(j, 2) * PIECE_C, PIECE_C)], slice(0, PIECE_C))]
        row, part, skip = (lax.div(j, 2), lax.rem(j, 2), 0) if phase == O_Q else (j, k, GROUP_COLS)
        return [(qkv.at[ds(row * PIECE_R, PIECE_R), ds(part * 4 * GROUP_COLS + skip + 2 * g * GROUP_COLS, GROUP_COLS)],
                 slice(g * GROUP_COLS, (g + 1) * GROUP_COLS)) for g in range(2)]

    def by_phase(t, low, high, phases, fn):
        for phase in phases:
            first, last = FIRST[phase], LAST[phase]
            if high < first or low >= last:
                continue
            if low >= first and high < last:
                fn(phase)
            else:
                pl.when((t >= first) & (t < last))(functools.partial(fn, phase))

    grads = (g_qkv, g_o, g_gate, g_up, g_down)
    moms = (m_qkv, m_o, m_gate, m_up, m_down)
    mom_news = (mn_qkv, mn_o, mn_gate, mn_up, mn_down)

    def waited(ref, sem):
        pltpu.make_async_copy(ref, ref, sem).wait()

    def load_grads(t, low, high):
        def start(phase):
            for k in range(2):
                for ref, cols in blocks(phase, k, t, grads):
                    pltpu.make_async_copy(ref, gbuf.at[lax.rem(t, 8), k, :, cols], g_sem.at[lax.rem(t, 8), k]).start()
        by_phase(t, low, high, range(4), start)

    def remote(src, dst, send, recv, where):
        return pltpu.make_async_remote_copy(src_ref=src, dst_ref=dst, send_sem=send, recv_sem=recv, device_id=where,
                                            device_id_type=MESH)

    def copies(k, t, which):
        s4, s8 = lax.rem(t, 4), lax.rem(t, 8)
        a, b = place[k]
        keep = ds(a * HALF_R + b * QUART_R, QUART_R)
        got = ds(a * HALF_R + (1 - b) * QUART_R, QUART_R)
        if which == 0:
            return remote(snd1.at[s4, k], r1.at[s8, k], send1.at[s4, k], recv1.at[s8, k], toward(k, 0))
        if which == 1:
            return remote(half.at[s4, k, ds((1 - b) * QUART_R, QUART_R)], r2.at[s8, k], send2.at[s4, k], recv2.at[s8, k], toward(k, 1))
        if which == 2:
            return remote(fin.at[s8, k, keep], fin.at[s8, k, keep], send3.at[s8, k], recv3.at[s8, k], toward(k, 1))
        if which == 3:
            return remote(fin.at[s8, k, keep], fin.at[s8, k, keep], send4.at[s8, k], recv4.at[s8, k], toward(k, 0))
        return remote(fin.at[s8, k, got], fin.at[s8, k, got], send5.at[s8, k], recv5.at[s8, k], toward(k, 0))

    def send_half(t, low, high):
        s4, s8 = lax.rem(t, 4), lax.rem(t, 8)
        for k in range(2):
            waited(gbuf.at[s8, k], g_sem.at[s8, k])
            a = place[k][0]
            snd1[s4, k] = gbuf[s8, k, ds((1 - a) * HALF_R, HALF_R), :].astype(F32)
            copies(k, t, 0).start()

    def send_quarter(t, low, high):
        s4, s8 = lax.rem(t, 4), lax.rem(t, 8)
        for k in range(2):
            copies(k, t, 0).wait()
            a = place[k][0]
            half[s4, k] = gbuf[s8, k, ds(a * HALF_R, HALF_R), :].astype(F32) + r1[s8, k]
            copies(k, t, 1).start()

    def share_quarter(t, low, high):
        s4, s8 = lax.rem(t, 4), lax.rem(t, 8)
        for k in range(2):
            copies(k, t, 1).wait()
            a, b = place[k]
            fin[s8, k, ds(a * HALF_R + b * QUART_R, QUART_R), :] = (half[s4, k, ds(b * QUART_R, QUART_R), :] + r2[s8, k]) * 0.25
            copies(k, t, 2).start()
            copies(k, t, 3).start()

    def pass_quarter(t, low, high):
        s4 = lax.rem(t, 4)
        for k in range(2):
            copies(k, t, 2).wait_recv()
            copies(k, t, 4).start()

        def start(phase):
            for k in range(2):
                for ref, cols in blocks(phase, k, t, moms):
                    pltpu.make_async_copy(ref, mbuf.at[s4, k, :, cols], m_sem.at[s4, k]).start()
        by_phase(t, low, high, range(4), start)

    def away_block(t, phase, k):
        j = t - FIRST[phase]
        s2 = lax.rem(t, 2)
        if phase == GATE_UP:
            src, rows, cols = nst.at[s2], ds(lax.div(j, 3) * PIECE_R, PIECE_R), ds(lax.rem(j, 3) * PIECE_C, PIECE_C)
        elif k == 0:
            src, rows, cols = nst_t.at[s2], ds(lax.rem(j, 2) * PIECE_C, PIECE_C), ds(lax.div(j, 2) * PIECE_R, PIECE_R)
        else:
            src, rows, cols = nst.at[s2], ds(lax.div(j, 2) * PIECE_R, PIECE_R), ds(lax.rem(j, 2) * PIECE_C, PIECE_C)
        return src, rows, cols

    def retire(t, low, high):
        s2, s4, s8 = lax.rem(t, 2), lax.rem(t, 4), lax.rem(t, 8)
        for k in range(2):
            copies(k, t, 2).wait_send()
            copies(k, t, 3).wait()
            copies(k, t, 4).wait()

        def finish(phase):
            if phase:
                @pl.when(t == FIRST[phase])
                def _():
                    pl.semaphore_wait(credit, 1)

                @pl.when(t > FIRST[phase])
                def _():
                    waited(nst.at[lax.rem(t + 1, 2)], nsend.at[lax.rem(t + 1, 2)])
            for k in range(2):
                waited(mbuf.at[s4, k], m_sem.at[s4, k])
                if phase:
                    waited(mst.at[s4, k], ms_sem.at[s4, k])
                else:
                    @pl.when(t >= 4)
                    def _():
                        waited(mst.at[s4, k], ms_sem.at[s4, k])
                mom_new, nest = moved_momentum(fin[s8, k], mbuf[s4, k])
                mst[s4, k] = mom_new
                for ref, cols in blocks(phase, k, t, mom_news):
                    pltpu.make_async_copy(mst.at[s4, k, :, cols], ref, ms_sem.at[s4, k]).start()
                if phase == DOWN:
                    rows, cols = pl.ds(k * PIECE_C, PIECE_C), ds(t * PIECE_R, PIECE_R)
                    nbuf[core, rows, cols] = nest.T
                    remote(nbuf.at[core, rows, cols], nbuf.at[core, rows, cols], dsend, nrecv.at[DOWN], {'tp': far}).start()
                    continue
                if phase == KEY_VALUE:
                    rows = ds((t - FIRST[KEY_VALUE]) * PIECE_R, PIECE_R)

                    def split(mine, nest=nest, k=k):
                        for g in range(2):
                            cols = slice((2 * k + g) * HEAD_DIM, (2 * k + g + 1) * HEAD_DIM)
                            heads = [nest[:, (2 * g + h) * HEAD_DIM:(2 * g + h + 1) * HEAD_DIM] for h in range(2)]
                            nbuf[core, rows, cols] = heads[mine]
                            nst[s2, :, cols] = heads[1 - mine]
                    pl.when(core == 0)(functools.partial(split, 0))
                    pl.when(core == 1)(functools.partial(split, 1))
                    if k:
                        remote(nst.at[s2], nbuf.at[core, rows, pl.ds(0, 2 * GROUP_COLS)], nsend.at[s2], nrecv.at[phase], {'tp': far}).start()
                    continue
                turned = phase == O_Q and k == 0
                piece = nest.T if turned else nest
                src, rows, cols = away_block(t, phase, k)

                @pl.when(core == k)
                def _():
                    nbuf[core, rows, cols] = piece

                @pl.when(core != k)
                def _():
                    (nst_t if turned else nst)[s2] = piece
                    remote(src, nbuf.at[core, rows, cols], nsend.at[s2], nrecv.at[phase], {'tp': far}).start()
        by_phase(t, low, high, range(4), finish)

    def service(s, low, high):
        for offset, stage in ((6, pass_quarter), (4, share_quarter), (2, send_quarter), (0, send_half), (8, retire), (-2, load_grads)):
            t, lo, hi = s - offset, low - offset, high - offset
            if hi < 0 or lo >= PAIRS:
                continue
            run = functools.partial(stage, t, max(lo, 0), min(hi, PAIRS - 1))
            guards = []
            if lo < 0:
                guards.append(t >= 0)
            if hi >= PAIRS:
                guards.append(t < PAIRS)
            if KV_DELAY and lo < FIRST[KEY_VALUE] and hi >= LAST[O_Q]:
                if lo >= LAST[O_Q] and hi < FIRST[KEY_VALUE]:
                    continue
                guards.append((t - LAST[O_Q]) * (t - FIRST[KEY_VALUE] + 1) > 0)
            if guards:
                pl.when(functools.reduce(jnp.logical_and, guards))(run)
            else:
                run()

    def services(low, high):
        def one(s, carry):
            service(s, low, high)
            return carry
        lax.fori_loop(low, high + 1, one, 0)

    def normalize(phase, w, x_out):
        waited(nbuf.at[far, :, pl.ds(0, w)], nrecv.at[phase])
        if phase == DOWN:
            waited(nbuf.at[core, :, pl.ds(0, w)], dsend)
        else:
            end = (LAST[phase] - 1) % 2
            waited(nst.at[end], nsend.at[end])
        rows_step = 64

        def square_rows(r, acc):
            rows = ds(r * rows_step, rows_step)
            a = nbuf[core, rows, :w]
            b = nbuf[far, rows, :w]
            return acc + (a * a + b * b)

        acc = lax.fori_loop(0, d // rows_step, square_rows, jnp.zeros((rows_step, w), F32))
        inv = 1.0 / (jnp.sqrt(jnp.sum(acc)) + EPSILON)

        def fill_rows(r, carry):
            rows = ds(r * rows_step, rows_step)
            x_out[rows, :w] = (nbuf[core, rows, :w] * inv).astype(BF16)
            x_out[rows, w:2 * w] = (nbuf[far, rows, :w] * inv).astype(BF16)
            return carry

        lax.fori_loop(0, d // rows_step, fill_rows, 0)

    def newton(phase, w, scale, first_service):
        normalize(phase, w, xbuf)
        pl.semaphore_signal(credit, inc=1, device_id={'tp': far}, device_id_type=MESH)

        def step(i, carry):
            block = BLOCK if phase == O_Q else PANEL
            gram_step(xbuf, 2 * w, s_ref, sb_ref, block)
            last = first_service + 2 * NEWTON_STEPS - 1
            service(first_service + 2 * i, first_service, last)
            poly_step(s_ref, sb_ref, t_ref, block)

            @pl.when(i < NEWTON_STEPS - 1)
            def _():
                def move(c, inner):
                    cols = ds(c * PANEL, PANEL)
                    xbuf[:, cols] = advanced(t_ref, xbuf, cols)
                    return inner
                lax.fori_loop(0, 2 * w // PANEL, move, 0)
            service(first_service + 2 * i + 1, first_service, last)
            return carry

        lax.fori_loop(0, NEWTON_STEPS, step, 0)
        count = w // PANEL
        if phase != DOWN:
            def return_copy(c):
                cols = slice((c % 2) * PANEL, (c % 2 + 1) * PANEL)
                return remote(s_ref.at[:, cols], xr.at[:, pl.ds(c * PANEL, PANEL)], xsend.at[c % 2], xrecv.at[phase], {'tp': far})

            for c in range(count):
                if c >= 2:
                    return_copy(c - 2).wait_send()
                s_ref[:, (c % 2) * PANEL:(c % 2 + 1) * PANEL] = advanced(t_ref, xbuf, pl.ds(w + c * PANEL, PANEL)).astype(F32)
                return_copy(c).start()

        def own(c, carry):
            cols = ds(c * PANEL, PANEL)
            xbuf[:, cols] = advanced(t_ref, xbuf, cols)
            return carry

        lax.fori_loop(0, count, own, 0)
        if phase != DOWN:
            for c in range(max(count - 2, 0), count):
                return_copy(c).wait_send()
            waited(xr.at[:, pl.ds(0, w)], xrecv.at[phase])

        def weights(k, weight, weight_new, kind, first=None):
            buf = wrow if kind == 'rows' else wcol
            count = w // 256

            def part(ref, i):
                if kind == 'rows':
                    return ref.at[ds(i * 256, 256), :]
                return ref.at[:, ds(i * 256, 256)]

            def load(i):
                return pltpu.make_async_copy(part(weight, i), buf.at[lax.rem(i, 3)], wl_sem.at[lax.rem(i, 3)])

            def store(i):
                return pltpu.make_async_copy(buf.at[lax.rem(i, 3)], part(weight_new, i), ws_sem.at[lax.rem(i, 3)])

            load(jnp.int32(0)).start()
            load(jnp.int32(1)).start()

            def one(i, carry):
                cols = ds(i * 256, 256)
                slot = lax.rem(i, 3)
                load(i).wait()

                def put(x_orth):
                    buf[slot] = weight_step(buf[slot], x_orth.T if kind == 'rows' else x_orth, scale)

                if phase == DOWN:
                    put(xbuf[:, cols].astype(F32))
                else:
                    @pl.when(core == k)
                    def _():
                        put(xbuf[:, cols].astype(F32))

                    @pl.when(core != k)
                    def _():
                        put(xr[:, cols])
                store(i).start()

                @pl.when(i >= 1)
                def _():
                    store(i - 1).wait()

                @pl.when(i + 2 < count)
                def _():
                    load(i + 2).start()
                if first is not None:
                    @pl.when(lax.rem(i, 3) == 2)
                    def _():
                        service(first + lax.div(i, 3), first, first + 1)
                return carry

            lax.fori_loop(0, count, one, 0)
            store(jnp.int32(count - 1)).wait()

        return weights

    load_grads(jnp.int32(0), 0, 0)
    load_grads(jnp.int32(1), 1, 1)
    services(0, 19)
    w_long, w_mid = w_gate.shape[1], w_o.shape[0]

    def scale_of(w):
        return 0.2 * math.sqrt(max(d, 2 * w))

    weights = newton(DOWN, w_long, scale_of(w_long), 20)
    weights(0, w_down, wn_down, 'rows', 30)
    services(32, 43)
    weights = newton(GATE_UP, w_long, scale_of(w_long), 44)
    weights(0, w_gate, wn_gate, 'cols', 54)
    weights(1, w_up, wn_up, 'cols')
    services(56, 59)
    newton(O_Q, w_mid, scale_of(w_mid), 60)
    handed = [pltpu.make_async_copy(xbuf.at[:, pl.ds(0, w_mid)], own_out, wl_sem.at[0]),
              pltpu.make_async_copy(xr.at[:, pl.ds(0, w_mid)], other_out, wl_sem.at[1])]
    for copy in handed:
        copy.start()
    services(70, PAIRS + 7)
    normalize(KEY_VALUE, 2 * GROUP_COLS, sb_ref)
    handed.append(pltpu.make_async_copy(sb_ref, kv_out, kv_sem))
    handed[-1].start()
    for slot in range(4):
        for k in range(2):
            waited(mst.at[slot, k], ms_sem.at[slot, k])
    for copy in handed:
        copy.wait()


def main_step(grads, weights, moms):
    any_spec = pl.BlockSpec(memory_space=pl.ANY)
    ins = list(grads) + list(weights) + list(moms)
    d, width = weights[0].shape
    outs = [jax.ShapeDtypeStruct(a.shape, F32) for a in list(weights[2:]) + list(moms)] + [
        jax.ShapeDtypeStruct((d, d), BF16), jax.ShapeDtypeStruct((d, weights[1].shape[0]), BF16),
        jax.ShapeDtypeStruct((d, weights[1].shape[0]), F32)]
    w_long = weights[2].shape[1]
    dma = pltpu.SemaphoreType.DMA
    pieces = (PIECE_R, PIECE_C)
    return pl.pallas_call(
        step_kernel,
        out_shape=outs,
        in_specs=[any_spec] * len(ins),
        out_specs=[any_spec] * len(outs),
        scratch_shapes=[
            pltpu.VMEM((2, d, w_long), F32), pltpu.VMEM((d, 2 * w_long), BF16), pltpu.VMEM((d, d), F32), pltpu.VMEM((d, d), BF16),
            pltpu.VMEM((d, d), BF16), pltpu.VMEM((d, w_long), F32), pltpu.VMEM((3, 256, d), F32), pltpu.VMEM((3, d, 256), F32),
            pltpu.VMEM((4, 2, HALF_R, PIECE_C), F32), pltpu.VMEM((4, 2, HALF_R, PIECE_C), F32),
            pltpu.VMEM((8, 2, HALF_R, PIECE_C), F32), pltpu.VMEM((8, 2, QUART_R, PIECE_C), F32), pltpu.VMEM((8, 2) + pieces, F32),
            pltpu.VMEM((8, 2) + pieces, BF16), pltpu.VMEM((4, 2) + pieces, F32), pltpu.VMEM((4, 2) + pieces, F32),
            pltpu.VMEM((2,) + pieces, F32), pltpu.VMEM((2, PIECE_C, PIECE_R), F32),
            dma((8, 2)), dma((4, 2)), dma((4, 2)), dma((4, 2)), dma((4, 2)), dma((8, 2)), dma((8, 2)), dma((8, 2)),
            dma((8, 2)), dma((8, 2)), dma((8, 2)), dma((8, 2)), dma((8, 2)),
            dma((2,)), dma, dma((4,)), dma((2,)), dma((3,)), dma((3,)), dma((3,)), dma, pltpu.SemaphoreType.REGULAR],
        compiler_params=pltpu.CompilerParams(vmem_limit_bytes=VMEM_BYTES, collective_id=0, has_side_effects=True),
        cost_estimate=pl.CostEstimate(flops=10 ** 11, bytes_accessed=2 * 10 ** 8, transcendentals=0),
    )(*ins)


def update_other(weight, x_back, weight_new, scale, core):
    rows, width = x_back.shape
    theirs = pl.BlockSpec((rows, HEAD_DIM), lambda g, c: (0, 4 * g + 3 - c[0]))

    def body(c_ref, w_ref, back_ref, unused, o_ref):
        o_ref[...] = weight_step(w_ref[...], back_ref[...], scale)

    moved = 12 * rows * width
    return pl.pallas_call(
        body, out_shape=jax.ShapeDtypeStruct(weight.shape, F32),
        grid_spec=pltpu.PrefetchScalarGridSpec(
            num_scalar_prefetch=1, grid=(width // HEAD_DIM,),
            in_specs=[theirs, pl.BlockSpec((rows, HEAD_DIM), lambda g, c: (0, g)), pl.BlockSpec(memory_space=pl.ANY)],
            out_specs=theirs),
        input_output_aliases={3: 0},
        compiler_params=pltpu.CompilerParams(vmem_limit_bytes=VMEM_BYTES),
        cost_estimate=pl.CostEstimate(flops=moved, bytes_accessed=moved, transcendentals=0),
    )(core, weight, x_back, weight_new)


def finish_kernel(*refs):
    x_in, own_in, other_in, w_qkv, w_o = refs[:5]
    srcs, out_far, wn_qkv, wn_o, dsts = refs[5:13], refs[13], refs[14], refs[15], refs[16:24]
    x_ref, x_own, s_ref, sb_ref, t_ref, wk = refs[24:30]
    bufs = refs[30:36]
    in_sem, out_sem, wl_sem, ws_sem, x_sem, step_sem, done_sem = refs[36:]
    d, w = out_far.shape
    load = pltpu.make_async_copy(x_in, x_ref, x_sem)
    load.start()
    core = lax.axis_index('tp')
    heads = [(g * HEAD_DIM, ds((4 * g + 2 + core) * HEAD_DIM, HEAD_DIM)) for g in range(w // HEAD_DIM)]
    scale = 0.2 * math.sqrt(max(d, 2 * w))
    for lo, at in heads:
        pltpu.make_async_copy(w_qkv.at[:, at], wk.at[:, lo:lo + HEAD_DIM], wl_sem).start()

    square = [buf.at[:d, :d] for buf in bufs]
    w_o_buf, w_q_buf, x_other = square[3:]
    queries = [(slice(g * GROUP_COLS, (g + 1) * GROUP_COLS), slice(2 * g * GROUP_COLS, (2 * g + 1) * GROUP_COLS))
               for g in range(d // GROUP_COLS)]
    loads = [pltpu.make_async_copy(other_in, x_other, step_sem.at[0]), pltpu.make_async_copy(own_in, x_own, step_sem.at[1]),
             pltpu.make_async_copy(w_o, w_o_buf, step_sem.at[2])]
    for copy in loads:
        copy.start()
    for near, at in queries:
        pltpu.make_async_copy(w_qkv.at[:, at], w_q_buf.at[:, near], step_sem.at[3]).start()
    moves = [(srcs[n], dsts[n]) for n in (2, 7, 0, 5, 1, 6, 4)] + [(srcs[3].at[:, lo:lo + d], dsts[3].at[:, lo:lo + d]) for lo in (0, d)]
    step_scale = 0.2 * math.sqrt(max(d, 2 * x_own.shape[1]))

    def held(n):
        return bufs[n] if n < 6 else square[n - 6]

    def fetch(n):
        if n >= 6:
            put_copy(n - 6).wait()
        pltpu.make_async_copy(moves[n][0], held(n), in_sem.at[n]).start()

    def put_copy(n):
        return pltpu.make_async_copy(held(n), moves[n][1], out_sem.at[n])

    def put(n):
        pltpu.make_async_copy(moves[n][0], held(n), in_sem.at[n]).wait()
        put_copy(n).start()

    def panels(mine, one):
        def loop(read):
            def body(c, carry):
                cols = ds(c * GROUP_COLS, GROUP_COLS)
                one(cols, read(cols))
                return carry
            lax.fori_loop(0, d // GROUP_COLS, body, 0)
        pl.when(core == mine)(lambda: loop(lambda cols: x_own[:, cols].astype(F32)))
        pl.when(core != mine)(lambda: loop(lambda cols: x_other[:, cols]))

    def step_o(unused):
        for copy in loads:
            copy.wait()

        def one(rows, x_orth):
            w_o_buf[rows, :] = weight_step(w_o_buf[rows, :], x_orth.T, step_scale)
        panels(0, one)
        pltpu.make_async_copy(w_o_buf, wn_o, done_sem.at[0]).start()

    def step_q(unused):
        pltpu.make_async_copy(w_q_buf, w_q_buf, step_sem.at[3]).wait()

        def one(cols, x_orth):
            w_q_buf[:, cols] = weight_step(w_q_buf[:, cols], x_orth, step_scale)
        panels(1, one)
        for near, at in queries:
            pltpu.make_async_copy(w_q_buf.at[:, near], wn_qkv.at[:, at], done_sem.at[1]).start()

    def freed(which):
        pltpu.make_async_copy((w_o_buf, w_q_buf)[which], (w_o_buf, w_q_buf)[which], done_sem.at[which]).wait()

    for n in range(3):
        fetch(n)
    plan = {(0, 2): ((step_o, 0), (put, 0)), (1, 0): ((step_q, 0), (put, 1), (fetch, 5)), (1, 1): ((put, 2),),
            (1, 2): ((freed, 0), (fetch, 3)), (2, 0): ((freed, 1), (fetch, 4), (fetch, 6)), (2, 1): ((put, 5), (fetch, 7)),
            (2, 2): ((put, 3), (fetch, 8)), (3, 0): ((put, 4),), (3, 1): ((put, 6),), (3, 2): ((put, 7),), (4, 0): ((put, 8),)}

    def step(i, carry):
        def at(slot):
            for turn in range(NEWTON_STEPS):
                if (turn, slot) in plan:
                    @pl.when(i == turn)
                    def _(todo=plan[turn, slot]):
                        for act, n in todo:
                            act(n)

        at(0)
        gram_step(x_ref, 2 * w, s_ref, sb_ref, BLOCK)
        at(1)
        poly_step(s_ref, sb_ref, t_ref, BLOCK)
        at(2)

        @pl.when(i < NEWTON_STEPS - 1)
        def _():
            def move(c, inner):
                cols = ds(c * PANEL, PANEL)
                x_ref[:, cols] = advanced(t_ref, x_ref, cols)
                return inner
            lax.fori_loop(0, 2 * w // PANEL, move, 0)
        return carry

    load.wait()
    lax.fori_loop(0, NEWTON_STEPS, step, 0)
    for c in range(w // PANEL):
        cols = slice(c * PANEL, (c + 1) * PANEL)
        out_far[:, cols] = advanced(t_ref, x_ref, pl.ds(w + c * PANEL, PANEL)).astype(F32)
    pltpu.make_async_copy(wk, wk, wl_sem).wait()
    for c in range(w // PANEL):
        cols = slice(c * PANEL, (c + 1) * PANEL)
        wk[:, cols] = weight_step(wk[:, cols], advanced(t_ref, x_ref, pl.ds(c * PANEL, PANEL)).astype(F32), scale)
    for lo, at in heads:
        pltpu.make_async_copy(wk.at[:, lo:lo + HEAD_DIM], wn_qkv.at[:, at], ws_sem).start()
    for n in range(3, 9):
        put_copy(n).wait()
    pltpu.make_async_copy(wk, wk, ws_sem).wait()


def finish(handed, w_qkv, w_o, arrays):
    d = handed[0].shape[0]
    w = handed[0].shape[1] // 2
    ins = list(handed) + [w_qkv, w_o] + list(arrays)
    any_spec = pl.BlockSpec(memory_space=pl.ANY)
    vmem = pl.BlockSpec(memory_space=pltpu.VMEM)
    dma = pltpu.SemaphoreType.DMA
    outs = [jax.ShapeDtypeStruct((d, w), F32)] + [jax.ShapeDtypeStruct(a.shape, F32) for a in [w_qkv, w_o] + list(arrays)]
    return pl.pallas_call(
        finish_kernel,
        out_shape=outs,
        in_specs=[any_spec] * len(ins),
        out_specs=[vmem] + [any_spec] * (len(outs) - 1),
        scratch_shapes=[pltpu.VMEM((d, d), BF16), pltpu.VMEM(handed[1].shape, BF16), pltpu.VMEM((d, d), F32), pltpu.VMEM((d, d), BF16),
                        pltpu.VMEM((d, d), BF16), pltpu.VMEM((d, w), F32)]
        + [pltpu.VMEM(arrays[n].shape, F32) for n in (2, 7, 0, 5, 1, 6)]
        + [dma((9,)), dma((9,)), dma, dma, dma, dma((4,)), dma((2,))],
        compiler_params=pltpu.CompilerParams(vmem_limit_bytes=VMEM_BYTES),
        cost_estimate=pl.CostEstimate(flops=3 * 10 ** 10, bytes_accessed=12 * 10 ** 7, transcendentals=0),
    )(*ins)


def solution(mesh):
    tp_count = mesh.shape['tp']
    col_spec = P(None, 'tp')
    row_spec = P('tp', None)
    grad_col = P('dp', None, 'tp')
    grad_row = P('dp', 'tp', None)
    weight_specs = (col_spec, row_spec, col_spec, col_spec, row_spec)
    in_specs = (grad_col, grad_row, grad_col, grad_col, grad_row) + weight_specs + weight_specs
    out_specs = weight_specs + weight_specs
    swap = [(0, 1), (1, 0)]

    def local_step(*arrays):
        weights, moms = arrays[5:10], arrays[10:]
        results = main_step([block[0] for block in arrays[:5]], weights, moms)
        done = finish(results[8:], weights[0], weights[1], results[:8])
        x_far, done = done[0], list(done[1:])
        scale = 0.2 * math.sqrt(max(x_far.shape[0], x_far.shape[1] * tp_count))
        core = lax.axis_index('tp').astype(jnp.int32).reshape(1)
        done[0] = update_other(weights[0], lax.ppermute(x_far, 'tp', swap), done[0], scale, core)
        return tuple(done)

    return jax.shard_map(local_step, mesh=mesh, in_specs=in_specs, out_specs=out_specs, check_vma=False)
```

```python
import functools
import math
import jax
import jax.numpy as jnp
from jax import lax
from jax.experimental import pallas as pl
from jax.experimental.pallas import tpu as pltpu
from jax.sharding import PartitionSpec as P

HEAD_DIM = 128
NEWTON_STEPS = 5
COEFF_A = 3.4445
COEFF_B = -4.7750
COEFF_C = 2.0315
MOMENTUM = 0.95
LEARN_RATE = 2e-3
WEIGHT_DECAY = 0.1
EPSILON = 1e-7
PANEL = 512
VMEM_BYTES = 67043328
F32 = jnp.float32
BF16 = jnp.bfloat16


GROUP_COLS = 2 * HEAD_DIM
MESH = pl.DeviceIdType.MESH
PIECE_R = 128
PIECE_C = 512
HALF_R = PIECE_R // 2
QUART_R = PIECE_R // 4
DOWN, GATE_UP, O_Q, KEY_VALUE = range(4)
KV_DELAY = 4
FIRST = (0, 12, 36, 52 + KV_DELAY)
LAST = (12, 36, 52, 60 + KV_DELAY)
PAIRS = LAST[-1]
BLOCK = 512


def ds(start, size):
    return pl.ds(start if isinstance(start, int) else pl.multiple_of(start, math.gcd(size, 128)), size)


def moved_momentum(grad, mom):
    mom_new = MOMENTUM * mom + grad
    return mom_new, grad + MOMENTUM * mom_new


def weight_step(weight, x_orth, scale):
    return weight - LEARN_RATE * (scale * x_orth + WEIGHT_DECAY * weight)


def gram_panel(x_ref, depth, j, block):
    return lax.dot_general(x_ref[:(j + 1) * block, :depth], x_ref[j * block:(j + 1) * block, :depth], (((1,), (1,)), ((), ())),
                           preferred_element_type=F32)


def gram_step(x_ref, depth, s_ref, sb_ref, block):
    for j in range(s_ref.shape[0] // block):
        cols = slice(j * block, (j + 1) * block)
        part = gram_panel(x_ref, depth, j, block)
        s_ref[:(j + 1) * block, cols] = part
        half = part.astype(BF16)
        sb_ref[:(j + 1) * block, cols] = half
        if j:
            sb_ref[cols, :j * block] = half[:j * block, :].T


def poly_step(s_ref, sb_ref, t_ref, block):
    for j in range(s_ref.shape[0] // block):
        cols = slice(j * block, (j + 1) * block)
        part = jnp.dot(sb_ref[:(j + 1) * block, :], sb_ref[:, cols], preferred_element_type=F32)
        poly_part = (COEFF_B * s_ref[:(j + 1) * block, cols] + COEFF_C * part).astype(BF16)
        t_ref[:(j + 1) * block, cols] = poly_part
        if j:
            t_ref[cols, :j * block] = poly_part[:j * block, :].T


def advanced(t_ref, x_ref, cols):
    x_cur = x_ref[:, cols]
    prod = jnp.dot(t_ref[...], x_cur, preferred_element_type=F32)
    return (COEFF_A * x_cur.astype(F32) + prod).astype(BF16)


def step_kernel(*refs):
    (g_qkv, g_o, g_gate, g_up, g_down, w_qkv, w_o, w_gate, w_up, w_down, m_qkv, m_o, m_gate, m_up, m_down,
     wn_gate, wn_up, wn_down, mn_qkv, mn_o, mn_gate, mn_up, mn_down, kv_out, own_out, other_out,
     nbuf, xbuf, s_ref, sb_ref, t_ref, xr, wrow, wcol, snd1, half, r1, r2, fin, gbuf, mbuf, mst, nst, nst_t,
     g_sem, m_sem, ms_sem, send1, send2, send3, send4, send5, recv1, recv2, recv3, recv4, recv5,
     nsend, dsend, nrecv, xsend, xrecv, wl_sem, ws_sem, kv_sem, credit) = refs
    dp = lax.axis_index('dp')
    core = lax.axis_index('tp')
    far = 1 - core
    pos_y, pos_x = lax.div(dp, 2), lax.rem(dp, 2)
    across = (pos_y * 2 + 1 - pos_x, (1 - pos_y) * 2 + pos_x)
    place = ((pos_x, pos_y), (pos_y, pos_x))
    d = s_ref.shape[0]

    def toward(k, second):
        return {'dp': across[k ^ second]}

    barrier = pltpu.get_barrier_semaphore()
    for where in ({'dp': across[0]}, {'dp': across[1]}, {'tp': far}):
        pl.semaphore_signal(barrier, inc=1, device_id=where, device_id_type=MESH)
    pl.semaphore_wait(barrier, 3)

    def blocks(phase, k, t, mats):
        j = t - FIRST[phase]
        qkv, o, gate, up, down = mats
        if phase == DOWN:
            return [(down.at[ds(j * PIECE_R, PIECE_R), pl.ds(k * PIECE_C, PIECE_C)], slice(0, PIECE_C))]
        if phase == GATE_UP:
            return [((gate, up)[k].at[ds(lax.div(j, 3) * PIECE_R, PIECE_R), ds(lax.rem(j, 3) * PIECE_C, PIECE_C)], slice(0, PIECE_C))]
        if phase == O_Q and k == 0:
            return [(o.at[ds(lax.div(j, 2) * PIECE_R, PIECE_R), ds(lax.rem(j, 2) * PIECE_C, PIECE_C)], slice(0, PIECE_C))]
        row, part, skip = (lax.div(j, 2), lax.rem(j, 2), 0) if phase == O_Q else (j, k, GROUP_COLS)
        return [(qkv.at[ds(row * PIECE_R, PIECE_R), ds(part * 4 * GROUP_COLS + skip + 2 * g * GROUP_COLS, GROUP_COLS)],
                 slice(g * GROUP_COLS, (g + 1) * GROUP_COLS)) for g in range(2)]

    def by_phase(t, low, high, phases, fn):
        for phase in phases:
            first, last = FIRST[phase], LAST[phase]
            if high < first or low >= last:
                continue
            if low >= first and high < last:
                fn(phase)
            else:
                pl.when((t >= first) & (t < last))(functools.partial(fn, phase))

    grads = (g_qkv, g_o, g_gate, g_up, g_down)
    moms = (m_qkv, m_o, m_gate, m_up, m_down)
    mom_news = (mn_qkv, mn_o, mn_gate, mn_up, mn_down)

    def waited(ref, sem):
        pltpu.make_async_copy(ref, ref, sem).wait()

    def load_grads(t, low, high):
        def start(phase):
            for k in range(2):
                for ref, cols in blocks(phase, k, t, grads):
                    pltpu.make_async_copy(ref, gbuf.at[lax.rem(t, 8), k, :, cols], g_sem.at[lax.rem(t, 8), k]).start()
        by_phase(t, low, high, range(4), start)

    def remote(src, dst, send, recv, where):
        return pltpu.make_async_remote_copy(src_ref=src, dst_ref=dst, send_sem=send, recv_sem=recv, device_id=where,
                                            device_id_type=MESH)

    def copies(k, t, which):
        s4, s8 = lax.rem(t, 4), lax.rem(t, 8)
        a, b = place[k]
        keep = ds(a * HALF_R + b * QUART_R, QUART_R)
        got = ds(a * HALF_R + (1 - b) * QUART_R, QUART_R)
        if which == 0:
            return remote(snd1.at[s4, k], r1.at[s8, k], send1.at[s4, k], recv1.at[s8, k], toward(k, 0))
        if which == 1:
            return remote(half.at[s4, k, ds((1 - b) * QUART_R, QUART_R)], r2.at[s8, k], send2.at[s4, k], recv2.at[s8, k], toward(k, 1))
        if which == 2:
            return remote(fin.at[s8, k, keep], fin.at[s8, k, keep], send3.at[s8, k], recv3.at[s8, k], toward(k, 1))
        if which == 3:
            return remote(fin.at[s8, k, keep], fin.at[s8, k, keep], send4.at[s8, k], recv4.at[s8, k], toward(k, 0))
        return remote(fin.at[s8, k, got], fin.at[s8, k, got], send5.at[s8, k], recv5.at[s8, k], toward(k, 0))

    def send_half(t, low, high):
        s4, s8 = lax.rem(t, 4), lax.rem(t, 8)
        for k in range(2):
            waited(gbuf.at[s8, k], g_sem.at[s8, k])
            a = place[k][0]
            snd1[s4, k] = gbuf[s8, k, ds((1 - a) * HALF_R, HALF_R), :].astype(F32)
            copies(k, t, 0).start()

    def send_quarter(t, low, high):
        s4, s8 = lax.rem(t, 4), lax.rem(t, 8)
        for k in range(2):
            copies(k, t, 0).wait()
            a = place[k][0]
            half[s4, k] = gbuf[s8, k, ds(a * HALF_R, HALF_R), :].astype(F32) + r1[s8, k]
            copies(k, t, 1).start()

    def share_quarter(t, low, high):
        s4, s8 = lax.rem(t, 4), lax.rem(t, 8)
        for k in range(2):
            copies(k, t, 1).wait()
            a, b = place[k]
            fin[s8, k, ds(a * HALF_R + b * QUART_R, QUART_R), :] = (half[s4, k, ds(b * QUART_R, QUART_R), :] + r2[s8, k]) * 0.25
            copies(k, t, 2).start()
            copies(k, t, 3).start()

    def pass_quarter(t, low, high):
        s4 = lax.rem(t, 4)
        for k in range(2):
            copies(k, t, 2).wait_recv()
            copies(k, t, 4).start()

        def start(phase):
            for k in range(2):
                for ref, cols in blocks(phase, k, t, moms):
                    pltpu.make_async_copy(ref, mbuf.at[s4, k, :, cols], m_sem.at[s4, k]).start()
        by_phase(t, low, high, range(4), start)

    def away_block(t, phase, k):
        j = t - FIRST[phase]
        s2 = lax.rem(t, 2)
        if phase == GATE_UP:
            src, rows, cols = nst.at[s2], ds(lax.div(j, 3) * PIECE_R, PIECE_R), ds(lax.rem(j, 3) * PIECE_C, PIECE_C)
        elif k == 0:
            src, rows, cols = nst_t.at[s2], ds(lax.rem(j, 2) * PIECE_C, PIECE_C), ds(lax.div(j, 2) * PIECE_R, PIECE_R)
        else:
            src, rows, cols = nst.at[s2], ds(lax.div(j, 2) * PIECE_R, PIECE_R), ds(lax.rem(j, 2) * PIECE_C, PIECE_C)
        return src, rows, cols

    def retire(t, low, high):
        s2, s4, s8 = lax.rem(t, 2), lax.rem(t, 4), lax.rem(t, 8)
        for k in range(2):
            copies(k, t, 2).wait_send()
            copies(k, t, 3).wait()
            copies(k, t, 4).wait()

        def finish(phase):
            if phase:
                @pl.when(t == FIRST[phase])
                def _():
                    pl.semaphore_wait(credit, 1)

                @pl.when(t > FIRST[phase])
                def _():
                    waited(nst.at[lax.rem(t + 1, 2)], nsend.at[lax.rem(t + 1, 2)])
            for k in range(2):
                waited(mbuf.at[s4, k], m_sem.at[s4, k])
                if phase:
                    waited(mst.at[s4, k], ms_sem.at[s4, k])
                else:
                    @pl.when(t >= 4)
                    def _():
                        waited(mst.at[s4, k], ms_sem.at[s4, k])
                mom_new, nest = moved_momentum(fin[s8, k], mbuf[s4, k])
                mst[s4, k] = mom_new
                for ref, cols in blocks(phase, k, t, mom_news):
                    pltpu.make_async_copy(mst.at[s4, k, :, cols], ref, ms_sem.at[s4, k]).start()
                if phase == DOWN:
                    rows, cols = pl.ds(k * PIECE_C, PIECE_C), ds(t * PIECE_R, PIECE_R)
                    nbuf[core, rows, cols] = nest.T
                    remote(nbuf.at[core, rows, cols], nbuf.at[core, rows, cols], dsend, nrecv.at[DOWN], {'tp': far}).start()
                    continue
                if phase == KEY_VALUE:
                    rows = ds((t - FIRST[KEY_VALUE]) * PIECE_R, PIECE_R)

                    def split(mine, nest=nest, k=k):
                        for g in range(2):
                            cols = slice((2 * k + g) * HEAD_DIM, (2 * k + g + 1) * HEAD_DIM)
                            heads = [nest[:, (2 * g + h) * HEAD_DIM:(2 * g + h + 1) * HEAD_DIM] for h in range(2)]
                            nbuf[core, rows, cols] = heads[mine]
                            nst[s2, :, cols] = heads[1 - mine]
                    pl.when(core == 0)(functools.partial(split, 0))
                    pl.when(core == 1)(functools.partial(split, 1))
                    if k:
                        remote(nst.at[s2], nbuf.at[core, rows, pl.ds(0, 2 * GROUP_COLS)], nsend.at[s2], nrecv.at[phase], {'tp': far}).start()
                    continue
                turned = phase == O_Q and k == 0
                piece = nest.T if turned else nest
                src, rows, cols = away_block(t, phase, k)

                @pl.when(core == k)
                def _():
                    nbuf[core, rows, cols] = piece

                @pl.when(core != k)
                def _():
                    (nst_t if turned else nst)[s2] = piece
                    remote(src, nbuf.at[core, rows, cols], nsend.at[s2], nrecv.at[phase], {'tp': far}).start()
        by_phase(t, low, high, range(4), finish)

    def service(s, low, high):
        for offset, stage in ((6, pass_quarter), (4, share_quarter), (2, send_quarter), (0, send_half), (8, retire), (-2, load_grads)):
            t, lo, hi = s - offset, low - offset, high - offset
            if hi < 0 or lo >= PAIRS:
                continue
            run = functools.partial(stage, t, max(lo, 0), min(hi, PAIRS - 1))
            guards = []
            if lo < 0:
                guards.append(t >= 0)
            if hi >= PAIRS:
                guards.append(t < PAIRS)
            if KV_DELAY and lo < FIRST[KEY_VALUE] and hi >= LAST[O_Q]:
                if lo >= LAST[O_Q] and hi < FIRST[KEY_VALUE]:
                    continue
                guards.append((t - LAST[O_Q]) * (t - FIRST[KEY_VALUE] + 1) > 0)
            if guards:
                pl.when(functools.reduce(jnp.logical_and, guards))(run)
            else:
                run()

    def services(low, high):
        def one(s, carry):
            service(s, low, high)
            return carry
        lax.fori_loop(low, high + 1, one, 0)

    def normalize(phase, w, x_out):
        waited(nbuf.at[far, :, pl.ds(0, w)], nrecv.at[phase])
        if phase == DOWN:
            waited(nbuf.at[core, :, pl.ds(0, w)], dsend)
        else:
            end = (LAST[phase] - 1) % 2
            waited(nst.at[end], nsend.at[end])
        rows_step = 64

        def square_rows(r, acc):
            rows = ds(r * rows_step, rows_step)
            a = nbuf[core, rows, :w]
            b = nbuf[far, rows, :w]
            return acc + (a * a + b * b)

        acc = lax.fori_loop(0, d // rows_step, square_rows, jnp.zeros((rows_step, w), F32))
        inv = 1.0 / (jnp.sqrt(jnp.sum(acc)) + EPSILON)

        def fill_rows(r, carry):
            rows = ds(r * rows_step, rows_step)
            x_out[rows, :w] = (nbuf[core, rows, :w] * inv).astype(BF16)
            x_out[rows, w:2 * w] = (nbuf[far, rows, :w] * inv).astype(BF16)
            return carry

        lax.fori_loop(0, d // rows_step, fill_rows, 0)

    def newton(phase, w, scale, first_service):
        normalize(phase, w, xbuf)
        pl.semaphore_signal(credit, inc=1, device_id={'tp': far}, device_id_type=MESH)

        def step(i, carry):
            block = BLOCK if phase == O_Q else PANEL
            gram_step(xbuf, 2 * w, s_ref, sb_ref, block)
            last = first_service + 2 * NEWTON_STEPS - 1
            service(first_service + 2 * i, first_service, last)
            poly_step(s_ref, sb_ref, t_ref, block)

            @pl.when(i < NEWTON_STEPS - 1)
            def _():
                def move(c, inner):
                    cols = ds(c * PANEL, PANEL)
                    xbuf[:, cols] = advanced(t_ref, xbuf, cols)
                    return inner
                lax.fori_loop(0, 2 * w // PANEL, move, 0)
            service(first_service + 2 * i + 1, first_service, last)
            return carry

        lax.fori_loop(0, NEWTON_STEPS, step, 0)
        count = w // PANEL
        if phase != DOWN:
            def return_copy(c):
                cols = slice((c % 2) * PANEL, (c % 2 + 1) * PANEL)
                return remote(s_ref.at[:, cols], xr.at[:, pl.ds(c * PANEL, PANEL)], xsend.at[c % 2], xrecv.at[phase], {'tp': far})

            for c in range(count):
                if c >= 2:
                    return_copy(c - 2).wait_send()
                s_ref[:, (c % 2) * PANEL:(c % 2 + 1) * PANEL] = advanced(t_ref, xbuf, pl.ds(w + c * PANEL, PANEL)).astype(F32)
                return_copy(c).start()

        def own(c, carry):
            cols = ds(c * PANEL, PANEL)
            xbuf[:, cols] = advanced(t_ref, xbuf, cols)
            return carry

        lax.fori_loop(0, count, own, 0)
        if phase != DOWN:
            for c in range(max(count - 2, 0), count):
                return_copy(c).wait_send()
            waited(xr.at[:, pl.ds(0, w)], xrecv.at[phase])

        def weights(k, weight, weight_new, kind, first=None):
            buf = wrow if kind == 'rows' else wcol
            count = w // 256

            def part(ref, i):
                if kind == 'rows':
                    return ref.at[ds(i * 256, 256), :]
                return ref.at[:, ds(i * 256, 256)]

            def load(i):
                return pltpu.make_async_copy(part(weight, i), buf.at[lax.rem(i, 3)], wl_sem.at[lax.rem(i, 3)])

            def store(i):
                return pltpu.make_async_copy(buf.at[lax.rem(i, 3)], part(weight_new, i), ws_sem.at[lax.rem(i, 3)])

            load(jnp.int32(0)).start()
            load(jnp.int32(1)).start()

            def one(i, carry):
                cols = ds(i * 256, 256)
                slot = lax.rem(i, 3)
                load(i).wait()

                def put(x_orth):
                    buf[slot] = weight_step(buf[slot], x_orth.T if kind == 'rows' else x_orth, scale)

                if phase == DOWN:
                    put(xbuf[:, cols].astype(F32))
                else:
                    @pl.when(core == k)
                    def _():
                        put(xbuf[:, cols].astype(F32))

                    @pl.when(core != k)
                    def _():
                        put(xr[:, cols])
                store(i).start()

                @pl.when(i >= 1)
                def _():
                    store(i - 1).wait()

                @pl.when(i + 2 < count)
                def _():
                    load(i + 2).start()
                if first is not None:
                    @pl.when(lax.rem(i, 3) == 2)
                    def _():
                        service(first + lax.div(i, 3), first, first + 1)
                return carry

            lax.fori_loop(0, count, one, 0)
            store(jnp.int32(count - 1)).wait()

        return weights

    load_grads(jnp.int32(0), 0, 0)
    load_grads(jnp.int32(1), 1, 1)
    services(0, 19)
    w_long, w_mid = w_gate.shape[1], w_o.shape[0]

    def scale_of(w):
        return 0.2 * math.sqrt(max(d, 2 * w))

    weights = newton(DOWN, w_long, scale_of(w_long), 20)
    weights(0, w_down, wn_down, 'rows', 30)
    services(32, 43)
    weights = newton(GATE_UP, w_long, scale_of(w_long), 44)
    weights(0, w_gate, wn_gate, 'cols', 54)
    weights(1, w_up, wn_up, 'cols')
    services(56, 59)
    newton(O_Q, w_mid, scale_of(w_mid), 60)
    handed = [pltpu.make_async_copy(xbuf.at[:, pl.ds(0, w_mid)], own_out, wl_sem.at[0]),
              pltpu.make_async_copy(xr.at[:, pl.ds(0, w_mid)], other_out, wl_sem.at[1])]
    for copy in handed:
        copy.start()
    services(70, PAIRS + 7)
    normalize(KEY_VALUE, 2 * GROUP_COLS, sb_ref)
    handed.append(pltpu.make_async_copy(sb_ref, kv_out, kv_sem))
    handed[-1].start()
    for slot in range(4):
        for k in range(2):
            waited(mst.at[slot, k], ms_sem.at[slot, k])
    for copy in handed:
        copy.wait()


def main_step(grads, weights, moms):
    any_spec = pl.BlockSpec(memory_space=pl.ANY)
    ins = list(grads) + list(weights) + list(moms)
    d, width = weights[0].shape
    outs = [jax.ShapeDtypeStruct(a.shape, F32) for a in list(weights[2:]) + list(moms)] + [
        jax.ShapeDtypeStruct((d, d), BF16), jax.ShapeDtypeStruct((d, weights[1].shape[0]), BF16),
        jax.ShapeDtypeStruct((d, weights[1].shape[0]), F32)]
    w_long = weights[2].shape[1]
    dma = pltpu.SemaphoreType.DMA
    pieces = (PIECE_R, PIECE_C)
    return pl.pallas_call(
        step_kernel,
        out_shape=outs,
        in_specs=[any_spec] * len(ins),
        out_specs=[any_spec] * len(outs),
        scratch_shapes=[
            pltpu.VMEM((2, d, w_long), F32), pltpu.VMEM((d, 2 * w_long), BF16), pltpu.VMEM((d, d), F32), pltpu.VMEM((d, d), BF16),
            pltpu.VMEM((d, d), BF16), pltpu.VMEM((d, w_long), F32), pltpu.VMEM((3, 256, d), F32), pltpu.VMEM((3, d, 256), F32),
            pltpu.VMEM((4, 2, HALF_R, PIECE_C), F32), pltpu.VMEM((4, 2, HALF_R, PIECE_C), F32),
            pltpu.VMEM((8, 2, HALF_R, PIECE_C), F32), pltpu.VMEM((8, 2, QUART_R, PIECE_C), F32), pltpu.VMEM((8, 2) + pieces, F32),
            pltpu.VMEM((8, 2) + pieces, BF16), pltpu.VMEM((4, 2) + pieces, F32), pltpu.VMEM((4, 2) + pieces, F32),
            pltpu.VMEM((2,) + pieces, F32), pltpu.VMEM((2, PIECE_C, PIECE_R), F32),
            dma((8, 2)), dma((4, 2)), dma((4, 2)), dma((4, 2)), dma((4, 2)), dma((8, 2)), dma((8, 2)), dma((8, 2)),
            dma((8, 2)), dma((8, 2)), dma((8, 2)), dma((8, 2)), dma((8, 2)),
            dma((2,)), dma, dma((4,)), dma((2,)), dma((3,)), dma((3,)), dma((3,)), dma, pltpu.SemaphoreType.REGULAR],
        compiler_params=pltpu.CompilerParams(vmem_limit_bytes=VMEM_BYTES, collective_id=0, has_side_effects=True),
        cost_estimate=pl.CostEstimate(flops=10 ** 11, bytes_accessed=2 * 10 ** 8, transcendentals=0),
    )(*ins)


def update_other(weight, x_back, weight_new, scale, core):
    rows, width = x_back.shape
    theirs = pl.BlockSpec((rows, HEAD_DIM), lambda g, c: (0, 4 * g + 3 - c[0]))

    def body(c_ref, w_ref, back_ref, unused, o_ref):
        o_ref[...] = weight_step(w_ref[...], back_ref[...], scale)

    moved = 12 * rows * width
    return pl.pallas_call(
        body, out_shape=jax.ShapeDtypeStruct(weight.shape, F32),
        grid_spec=pltpu.PrefetchScalarGridSpec(
            num_scalar_prefetch=1, grid=(width // HEAD_DIM,),
            in_specs=[theirs, pl.BlockSpec((rows, HEAD_DIM), lambda g, c: (0, g)), pl.BlockSpec(memory_space=pl.ANY)],
            out_specs=theirs),
        input_output_aliases={3: 0},
        compiler_params=pltpu.CompilerParams(vmem_limit_bytes=VMEM_BYTES),
        cost_estimate=pl.CostEstimate(flops=moved, bytes_accessed=moved, transcendentals=0),
    )(core, weight, x_back, weight_new)


def finish_kernel(*refs):
    x_in, own_in, other_in, w_qkv, w_o = refs[:5]
    srcs, out_far, wn_qkv, wn_o, dsts = refs[5:13], refs[13], refs[14], refs[15], refs[16:24]
    x_ref, x_own, s_ref, sb_ref, t_ref, wk = refs[24:30]
    bufs = refs[30:36]
    in_sem, out_sem, wl_sem, ws_sem, x_sem, step_sem, done_sem = refs[36:]
    d, w = out_far.shape
    load = pltpu.make_async_copy(x_in, x_ref, x_sem)
    load.start()
    core = lax.axis_index('tp')
    heads = [(g * HEAD_DIM, ds((4 * g + 2 + core) * HEAD_DIM, HEAD_DIM)) for g in range(w // HEAD_DIM)]
    scale = 0.2 * math.sqrt(max(d, 2 * w))
    for lo, at in heads:
        pltpu.make_async_copy(w_qkv.at[:, at], wk.at[:, lo:lo + HEAD_DIM], wl_sem).start()

    square = [buf.at[:d, :d] for buf in bufs]
    w_o_buf, w_q_buf, x_other = square[3:]
    queries = [(slice(g * GROUP_COLS, (g + 1) * GROUP_COLS), slice(2 * g * GROUP_COLS, (2 * g + 1) * GROUP_COLS))
               for g in range(d // GROUP_COLS)]
    moves = [(srcs[n], dsts[n]) for n in (2, 7, 0, 5, 1, 6, 4)] + [(srcs[3].at[:, lo:lo + d], dsts[3].at[:, lo:lo + d]) for lo in (0, d)]
    step_scale = 0.2 * math.sqrt(max(d, 2 * x_own.shape[1]))

    def held(n):
        return bufs[n] if n < 6 else square[n - 6]

    def fetch(n):
        if n >= 6:
            put_copy(n - 6).wait()
        pltpu.make_async_copy(moves[n][0], held(n), in_sem.at[n]).start()

    def put_copy(n):
        return pltpu.make_async_copy(held(n), moves[n][1], out_sem.at[n])

    def put(n):
        pltpu.make_async_copy(moves[n][0], held(n), in_sem.at[n]).wait()
        put_copy(n).start()

    for n in range(3):
        fetch(n)
    loads = [pltpu.make_async_copy(other_in, x_other, step_sem.at[0]), pltpu.make_async_copy(own_in, x_own, step_sem.at[1]),
             pltpu.make_async_copy(w_o, w_o_buf, step_sem.at[2])]
    for copy in loads:
        copy.start()
    for near, at in queries:
        pltpu.make_async_copy(w_qkv.at[:, at], w_q_buf.at[:, near], step_sem.at[3]).start()

    def panels(mine, one):
        def loop(read):
            def body(c, carry):
                cols = ds(c * GROUP_COLS, GROUP_COLS)
                one(cols, read(cols))
                return carry
            lax.fori_loop(0, d // GROUP_COLS, body, 0)
        pl.when(core == mine)(lambda: loop(lambda cols: x_own[:, cols].astype(F32)))
        pl.when(core != mine)(lambda: loop(lambda cols: x_other[:, cols]))

    def step_o(unused):
        for copy in loads:
            copy.wait()

        def one(rows, x_orth):
            w_o_buf[rows, :] = weight_step(w_o_buf[rows, :], x_orth.T, step_scale)
        panels(0, one)
        pltpu.make_async_copy(w_o_buf, wn_o, done_sem.at[0]).start()

    def step_q(unused):
        pltpu.make_async_copy(w_q_buf, w_q_buf, step_sem.at[3]).wait()

        def one(cols, x_orth):
            w_q_buf[:, cols] = weight_step(w_q_buf[:, cols], x_orth, step_scale)
        panels(1, one)
        for near, at in queries:
            pltpu.make_async_copy(w_q_buf.at[:, near], wn_qkv.at[:, at], done_sem.at[1]).start()

    def freed(which):
        pltpu.make_async_copy((w_o_buf, w_q_buf)[which], (w_o_buf, w_q_buf)[which], done_sem.at[which]).wait()

    plan = {(0, 1): ((put, 0),), (0, 2): ((put, 1),), (1, 0): ((put, 2), (fetch, 6)), (1, 1): ((step_o, 0), (fetch, 7)),
            (1, 2): ((step_q, 0), (fetch, 5), (fetch, 8)), (2, 0): ((freed, 0), (fetch, 3), (freed, 1), (fetch, 4), (put, 6)),
            (2, 1): ((put, 7),), (2, 2): ((put, 5),), (3, 0): ((put, 8),), (3, 1): ((put, 3),), (3, 2): ((put, 4),)}

    def step(i, carry):
        def at(slot):
            for turn in range(NEWTON_STEPS):
                if (turn, slot) in plan:
                    @pl.when(i == turn)
                    def _(todo=plan[turn, slot]):
                        for act, n in todo:
                            act(n)

        at(0)
        gram_step(x_ref, 2 * w, s_ref, sb_ref, BLOCK)
        at(1)
        poly_step(s_ref, sb_ref, t_ref, BLOCK)
        at(2)

        @pl.when(i < NEWTON_STEPS - 1)
        def _():
            def move(c, inner):
                cols = ds(c * PANEL, PANEL)
                x_ref[:, cols] = advanced(t_ref, x_ref, cols)
                return inner
            lax.fori_loop(0, 2 * w // PANEL, move, 0)
        return carry

    load.wait()
    lax.fori_loop(0, NEWTON_STEPS, step, 0)
    for c in range(w // PANEL):
        cols = slice(c * PANEL, (c + 1) * PANEL)
        out_far[:, cols] = advanced(t_ref, x_ref, pl.ds(w + c * PANEL, PANEL)).astype(F32)
    pltpu.make_async_copy(wk, wk, wl_sem).wait()
    for c in range(w // PANEL):
        cols = slice(c * PANEL, (c + 1) * PANEL)
        wk[:, cols] = weight_step(wk[:, cols], advanced(t_ref, x_ref, pl.ds(c * PANEL, PANEL)).astype(F32), scale)
    for lo, at in heads:
        pltpu.make_async_copy(wk.at[:, lo:lo + HEAD_DIM], wn_qkv.at[:, at], ws_sem).start()
    for n in range(3, 9):
        put_copy(n).wait()
    pltpu.make_async_copy(wk, wk, ws_sem).wait()


def finish(handed, w_qkv, w_o, arrays):
    d = handed[0].shape[0]
    w = handed[0].shape[1] // 2
    ins = list(handed) + [w_qkv, w_o] + list(arrays)
    any_spec = pl.BlockSpec(memory_space=pl.ANY)
    vmem = pl.BlockSpec(memory_space=pltpu.VMEM)
    dma = pltpu.SemaphoreType.DMA
    outs = [jax.ShapeDtypeStruct((d, w), F32)] + [jax.ShapeDtypeStruct(a.shape, F32) for a in [w_qkv, w_o] + list(arrays)]
    return pl.pallas_call(
        finish_kernel,
        out_shape=outs,
        in_specs=[any_spec] * len(ins),
        out_specs=[vmem] + [any_spec] * (len(outs) - 1),
        scratch_shapes=[pltpu.VMEM((d, d), BF16), pltpu.VMEM(handed[1].shape, BF16), pltpu.VMEM((d, d), F32), pltpu.VMEM((d, d), BF16),
                        pltpu.VMEM((d, d), BF16), pltpu.VMEM((d, w), F32)]
        + [pltpu.VMEM(arrays[n].shape, F32) for n in (2, 7, 0, 5, 1, 6)]
        + [dma((9,)), dma((9,)), dma, dma, dma, dma((4,)), dma((2,))],
        compiler_params=pltpu.CompilerParams(vmem_limit_bytes=VMEM_BYTES),
        cost_estimate=pl.CostEstimate(flops=3 * 10 ** 10, bytes_accessed=12 * 10 ** 7, transcendentals=0),
    )(*ins)


def solution(mesh):
    tp_count = mesh.shape['tp']
    col_spec = P(None, 'tp')
    row_spec = P('tp', None)
    grad_col = P('dp', None, 'tp')
    grad_row = P('dp', 'tp', None)
    weight_specs = (col_spec, row_spec, col_spec, col_spec, row_spec)
    in_specs = (grad_col, grad_row, grad_col, grad_col, grad_row) + weight_specs + weight_specs
    out_specs = weight_specs + weight_specs
    swap = [(0, 1), (1, 0)]

    def local_step(*arrays):
        weights, moms = arrays[5:10], arrays[10:]
        results = main_step([block[0] for block in arrays[:5]], weights, moms)
        done = finish(results[8:], weights[0], weights[1], results[:8])
        x_far, done = done[0], list(done[1:])
        scale = 0.2 * math.sqrt(max(x_far.shape[0], x_far.shape[1] * tp_count))
        core = lax.axis_index('tp').astype(jnp.int32).reshape(1)
        done[0] = update_other(weights[0], lax.ppermute(x_far, 'tp', swap), done[0], scale, core)
        return tuple(done)

    return jax.shard_map(local_step, mesh=mesh, in_specs=in_specs, out_specs=out_specs, check_vma=False)
```

```python
import functools
import math
import jax
import jax.numpy as jnp
from jax import lax
from jax.experimental import pallas as pl
from jax.experimental.pallas import tpu as pltpu
from jax.sharding import PartitionSpec as P

HEAD_DIM = 128
NEWTON_STEPS = 5
COEFF_A = 3.4445
COEFF_B = -4.7750
COEFF_C = 2.0315
MOMENTUM = 0.95
LEARN_RATE = 2e-3
WEIGHT_DECAY = 0.1
EPSILON = 1e-7
PANEL = 512
VMEM_BYTES = 67043328
F32 = jnp.float32
BF16 = jnp.bfloat16


GROUP_COLS = 2 * HEAD_DIM
MESH = pl.DeviceIdType.MESH
PIECE_R = 128
PIECE_C = 512
HALF_R = PIECE_R // 2
QUART_R = PIECE_R // 4
DOWN, GATE_UP, O_Q, KEY_VALUE = range(4)
KV_DELAY = 4
FIRST = (0, 12, 36, 52 + KV_DELAY)
LAST = (12, 36, 52, 60 + KV_DELAY)
PAIRS = LAST[-1]
BLOCK = 512


def ds(start, size):
    return pl.ds(start if isinstance(start, int) else pl.multiple_of(start, math.gcd(size, 128)), size)


def moved_momentum(grad, mom):
    mom_new = MOMENTUM * mom + grad
    return mom_new, grad + MOMENTUM * mom_new


def weight_step(weight, x_orth, scale):
    return weight - LEARN_RATE * (scale * x_orth + WEIGHT_DECAY * weight)


def gram_panel(x_ref, depth, j, block):
    return lax.dot_general(x_ref[:(j + 1) * block, :depth], x_ref[j * block:(j + 1) * block, :depth], (((1,), (1,)), ((), ())),
                           preferred_element_type=F32)


def gram_step(x_ref, depth, s_ref, sb_ref, block):
    for j in range(s_ref.shape[0] // block):
        cols = slice(j * block, (j + 1) * block)
        part = gram_panel(x_ref, depth, j, block)
        s_ref[:(j + 1) * block, cols] = part
        half = part.astype(BF16)
        sb_ref[:(j + 1) * block, cols] = half
        if j:
            sb_ref[cols, :j * block] = half[:j * block, :].T


def poly_step(s_ref, sb_ref, t_ref, block):
    for j in range(s_ref.shape[0] // block):
        cols = slice(j * block, (j + 1) * block)
        part = jnp.dot(sb_ref[:(j + 1) * block, :], sb_ref[:, cols], preferred_element_type=F32)
        poly_part = (COEFF_B * s_ref[:(j + 1) * block, cols] + COEFF_C * part).astype(BF16)
        t_ref[:(j + 1) * block, cols] = poly_part
        if j:
            t_ref[cols, :j * block] = poly_part[:j * block, :].T


def advanced(t_ref, x_ref, cols):
    x_cur = x_ref[:, cols]
    prod = jnp.dot(t_ref[...], x_cur, preferred_element_type=F32)
    return (COEFF_A * x_cur.astype(F32) + prod).astype(BF16)


def step_kernel(*refs):
    (g_qkv, g_o, g_gate, g_up, g_down, w_qkv, w_o, w_gate, w_up, w_down, m_qkv, m_o, m_gate, m_up, m_down,
     wn_gate, wn_up, wn_down, mn_qkv, mn_o, mn_gate, mn_up, mn_down, kv_out, own_out, other_out,
     nbuf, xbuf, s_ref, sb_ref, t_ref, xr, wrow, wcol, snd1, half, r1, r2, fin, gbuf, mbuf, mst, nst, nst_t,
     g_sem, m_sem, ms_sem, send1, send2, send3, send4, send5, recv1, recv2, recv3, recv4, recv5,
     nsend, dsend, nrecv, xsend, xrecv, wl_sem, ws_sem, kv_sem, credit) = refs
    dp = lax.axis_index('dp')
    core = lax.axis_index('tp')
    far = 1 - core
    pos_y, pos_x = lax.div(dp, 2), lax.rem(dp, 2)
    across = (pos_y * 2 + 1 - pos_x, (1 - pos_y) * 2 + pos_x)
    place = ((pos_x, pos_y), (pos_y, pos_x))
    d = s_ref.shape[0]

    def toward(k, second):
        return {'dp': across[k ^ second]}

    barrier = pltpu.get_barrier_semaphore()
    for where in ({'dp': across[0]}, {'dp': across[1]}, {'tp': far}):
        pl.semaphore_signal(barrier, inc=1, device_id=where, device_id_type=MESH)
    pl.semaphore_wait(barrier, 3)

    def blocks(phase, k, t, mats):
        j = t - FIRST[phase]
        qkv, o, gate, up, down = mats
        if phase == DOWN:
            return [(down.at[ds(j * PIECE_R, PIECE_R), pl.ds(k * PIECE_C, PIECE_C)], slice(0, PIECE_C))]
        if phase == GATE_UP:
            return [((gate, up)[k].at[ds(lax.div(j, 3) * PIECE_R, PIECE_R), ds(lax.rem(j, 3) * PIECE_C, PIECE_C)], slice(0, PIECE_C))]
        if phase == O_Q and k == 0:
            return [(o.at[ds(lax.div(j, 2) * PIECE_R, PIECE_R), ds(lax.rem(j, 2) * PIECE_C, PIECE_C)], slice(0, PIECE_C))]
        row, part, skip = (lax.div(j, 2), lax.rem(j, 2), 0) if phase == O_Q else (j, k, GROUP_COLS)
        return [(qkv.at[ds(row * PIECE_R, PIECE_R), ds(part * 4 * GROUP_COLS + skip + 2 * g * GROUP_COLS, GROUP_COLS)],
                 slice(g * GROUP_COLS, (g + 1) * GROUP_COLS)) for g in range(2)]

    def by_phase(t, low, high, phases, fn):
        for phase in phases:
            first, last = FIRST[phase], LAST[phase]
            if high < first or low >= last:
                continue
            if low >= first and high < last:
                fn(phase)
            else:
                pl.when((t >= first) & (t < last))(functools.partial(fn, phase))

    grads = (g_qkv, g_o, g_gate, g_up, g_down)
    moms = (m_qkv, m_o, m_gate, m_up, m_down)
    mom_news = (mn_qkv, mn_o, mn_gate, mn_up, mn_down)

    def waited(ref, sem):
        pltpu.make_async_copy(ref, ref, sem).wait()

    def load_grads(t, low, high):
        def start(phase):
            for k in range(2):
                for ref, cols in blocks(phase, k, t, grads):
                    pltpu.make_async_copy(ref, gbuf.at[lax.rem(t, 8), k, :, cols], g_sem.at[lax.rem(t, 8), k]).start()
        by_phase(t, low, high, range(4), start)

    def remote(src, dst, send, recv, where):
        return pltpu.make_async_remote_copy(src_ref=src, dst_ref=dst, send_sem=send, recv_sem=recv, device_id=where,
                                            device_id_type=MESH)

    def copies(k, t, which):
        s4, s8 = lax.rem(t, 4), lax.rem(t, 8)
        a, b = place[k]
        keep = ds(a * HALF_R + b * QUART_R, QUART_R)
        got = ds(a * HALF_R + (1 - b) * QUART_R, QUART_R)
        if which == 0:
            return remote(snd1.at[s4, k], r1.at[s8, k], send1.at[s4, k], recv1.at[s8, k], toward(k, 0))
        if which == 1:
            return remote(half.at[s4, k, ds((1 - b) * QUART_R, QUART_R)], r2.at[s8, k], send2.at[s4, k], recv2.at[s8, k], toward(k, 1))
        if which == 2:
            return remote(fin.at[s8, k, keep], fin.at[s8, k, keep], send3.at[s8, k], recv3.at[s8, k], toward(k, 1))
        if which == 3:
            return remote(fin.at[s8, k, keep], fin.at[s8, k, keep], send4.at[s8, k], recv4.at[s8, k], toward(k, 0))
        return remote(fin.at[s8, k, got], fin.at[s8, k, got], send5.at[s8, k], recv5.at[s8, k], toward(k, 0))

    def send_half(t, low, high):
        s4, s8 = lax.rem(t, 4), lax.rem(t, 8)
        for k in range(2):
            waited(gbuf.at[s8, k], g_sem.at[s8, k])
            a = place[k][0]
            snd1[s4, k] = gbuf[s8, k, ds((1 - a) * HALF_R, HALF_R), :].astype(F32)
            copies(k, t, 0).start()

    def send_quarter(t, low, high):
        s4, s8 = lax.rem(t, 4), lax.rem(t, 8)
        for k in range(2):
            copies(k, t, 0).wait()
            a = place[k][0]
            half[s4, k] = gbuf[s8, k, ds(a * HALF_R, HALF_R), :].astype(F32) + r1[s8, k]
            copies(k, t, 1).start()

    def share_quarter(t, low, high):
        s4, s8 = lax.rem(t, 4), lax.rem(t, 8)
        for k in range(2):
            copies(k, t, 1).wait()
            a, b = place[k]
            fin[s8, k, ds(a * HALF_R + b * QUART_R, QUART_R), :] = (half[s4, k, ds(b * QUART_R, QUART_R), :] + r2[s8, k]) * 0.25
            copies(k, t, 2).start()
            copies(k, t, 3).start()

    def pass_quarter(t, low, high):
        s4 = lax.rem(t, 4)
        for k in range(2):
            copies(k, t, 2).wait_recv()
            copies(k, t, 4).start()

        def start(phase):
            for k in range(2):
                for ref, cols in blocks(phase, k, t, moms):
                    pltpu.make_async_copy(ref, mbuf.at[s4, k, :, cols], m_sem.at[s4, k]).start()
        by_phase(t, low, high, range(4), start)

    def away_block(t, phase, k):
        j = t - FIRST[phase]
        s2 = lax.rem(t, 2)
        if phase == GATE_UP:
            src, rows, cols = nst.at[s2], ds(lax.div(j, 3) * PIECE_R, PIECE_R), ds(lax.rem(j, 3) * PIECE_C, PIECE_C)
        elif k == 0:
            src, rows, cols = nst_t.at[s2], ds(lax.rem(j, 2) * PIECE_C, PIECE_C), ds(lax.div(j, 2) * PIECE_R, PIECE_R)
        else:
            src, rows, cols = nst.at[s2], ds(lax.div(j, 2) * PIECE_R, PIECE_R), ds(lax.rem(j, 2) * PIECE_C, PIECE_C)
        return src, rows, cols

    def retire(t, low, high):
        s2, s4, s8 = lax.rem(t, 2), lax.rem(t, 4), lax.rem(t, 8)
        for k in range(2):
            copies(k, t, 2).wait_send()
            copies(k, t, 3).wait()
            copies(k, t, 4).wait()

        def finish(phase):
            if phase:
                @pl.when(t == FIRST[phase])
                def _():
                    pl.semaphore_wait(credit, 1)

                @pl.when(t > FIRST[phase])
                def _():
                    waited(nst.at[lax.rem(t + 1, 2)], nsend.at[lax.rem(t + 1, 2)])
            for k in range(2):
                waited(mbuf.at[s4, k], m_sem.at[s4, k])
                if phase:
                    waited(mst.at[s4, k], ms_sem.at[s4, k])
                else:
                    @pl.when(t >= 4)
                    def _():
                        waited(mst.at[s4, k], ms_sem.at[s4, k])
                mom_new, nest = moved_momentum(fin[s8, k], mbuf[s4, k])
                mst[s4, k] = mom_new
                for ref, cols in blocks(phase, k, t, mom_news):
                    pltpu.make_async_copy(mst.at[s4, k, :, cols], ref, ms_sem.at[s4, k]).start()
                if phase == DOWN:
                    rows, cols = pl.ds(k * PIECE_C, PIECE_C), ds(t * PIECE_R, PIECE_R)
                    nbuf[core, rows, cols] = nest.T
                    remote(nbuf.at[core, rows, cols], nbuf.at[core, rows, cols], dsend, nrecv.at[DOWN], {'tp': far}).start()
                    continue
                if phase == KEY_VALUE:
                    rows = ds((t - FIRST[KEY_VALUE]) * PIECE_R, PIECE_R)

                    def split(mine, nest=nest, k=k):
                        for g in range(2):
                            cols = slice((2 * k + g) * HEAD_DIM, (2 * k + g + 1) * HEAD_DIM)
                            heads = [nest[:, (2 * g + h) * HEAD_DIM:(2 * g + h + 1) * HEAD_DIM] for h in range(2)]
                            nbuf[core, rows, cols] = heads[mine]
                            nst[s2, :, cols] = heads[1 - mine]
                    pl.when(core == 0)(functools.partial(split, 0))
                    pl.when(core == 1)(functools.partial(split, 1))
                    if k:
                        remote(nst.at[s2], nbuf.at[core, rows, pl.ds(0, 2 * GROUP_COLS)], nsend.at[s2], nrecv.at[phase], {'tp': far}).start()
                    continue
                turned = phase == O_Q and k == 0
                piece = nest.T if turned else nest
                src, rows, cols = away_block(t, phase, k)

                @pl.when(core == k)
                def _():
                    nbuf[core, rows, cols] = piece

                @pl.when(core != k)
                def _():
                    (nst_t if turned else nst)[s2] = piece
                    remote(src, nbuf.at[core, rows, cols], nsend.at[s2], nrecv.at[phase], {'tp': far}).start()
        by_phase(t, low, high, range(4), finish)

    def service(s, low, high):
        for offset, stage in ((6, pass_quarter), (4, share_quarter), (2, send_quarter), (0, send_half), (8, retire), (-2, load_grads)):
            t, lo, hi = s - offset, low - offset, high - offset
            if hi < 0 or lo >= PAIRS:
                continue
            run = functools.partial(stage, t, max(lo, 0), min(hi, PAIRS - 1))
            guards = []
            if lo < 0:
                guards.append(t >= 0)
            if hi >= PAIRS:
                guards.append(t < PAIRS)
            if KV_DELAY and lo < FIRST[KEY_VALUE] and hi >= LAST[O_Q]:
                if lo >= LAST[O_Q] and hi < FIRST[KEY_VALUE]:
                    continue
                guards.append((t - LAST[O_Q]) * (t - FIRST[KEY_VALUE] + 1) > 0)
            if guards:
                pl.when(functools.reduce(jnp.logical_and, guards))(run)
            else:
                run()

    def services(low, high):
        def one(s, carry):
            service(s, low, high)
            return carry
        lax.fori_loop(low, high + 1, one, 0)

    def normalize(phase, w, x_out):
        waited(nbuf.at[far, :, pl.ds(0, w)], nrecv.at[phase])
        if phase == DOWN:
            waited(nbuf.at[core, :, pl.ds(0, w)], dsend)
        else:
            end = (LAST[phase] - 1) % 2
            waited(nst.at[end], nsend.at[end])
        rows_step = 64

        def square_rows(r, acc):
            rows = ds(r * rows_step, rows_step)
            a = nbuf[core, rows, :w]
            b = nbuf[far, rows, :w]
            return acc + (a * a + b * b)

        acc = lax.fori_loop(0, d // rows_step, square_rows, jnp.zeros((rows_step, w), F32))
        inv = 1.0 / (jnp.sqrt(jnp.sum(acc)) + EPSILON)

        def fill_rows(r, carry):
            rows = ds(r * rows_step, rows_step)
            x_out[rows, :w] = (nbuf[core, rows, :w] * inv).astype(BF16)
            x_out[rows, w:2 * w] = (nbuf[far, rows, :w] * inv).astype(BF16)
            return carry

        lax.fori_loop(0, d // rows_step, fill_rows, 0)

    def newton(phase, w, scale, first_service):
        normalize(phase, w, xbuf)
        pl.semaphore_signal(credit, inc=1, device_id={'tp': far}, device_id_type=MESH)

        def step(i, carry):
            block = BLOCK if phase == O_Q else PANEL
            gram_step(xbuf, 2 * w, s_ref, sb_ref, block)
            last = first_service + 2 * NEWTON_STEPS - 1
            service(first_service + 2 * i, first_service, last)
            poly_step(s_ref, sb_ref, t_ref, block)

            @pl.when(i < NEWTON_STEPS - 1)
            def _():
                def move(c, inner):
                    cols = ds(c * PANEL, PANEL)
                    xbuf[:, cols] = advanced(t_ref, xbuf, cols)
                    return inner
                lax.fori_loop(0, 2 * w // PANEL, move, 0)
            service(first_service + 2 * i + 1, first_service, last)
            return carry

        lax.fori_loop(0, NEWTON_STEPS, step, 0)
        count = w // PANEL
        if phase != DOWN:
            def return_copy(c):
                cols = slice((c % 2) * PANEL, (c % 2 + 1) * PANEL)
                return remote(s_ref.at[:, cols], xr.at[:, pl.ds(c * PANEL, PANEL)], xsend.at[c % 2], xrecv.at[phase], {'tp': far})

            for c in range(count):
                if c >= 2:
                    return_copy(c - 2).wait_send()
                s_ref[:, (c % 2) * PANEL:(c % 2 + 1) * PANEL] = advanced(t_ref, xbuf, pl.ds(w + c * PANEL, PANEL)).astype(F32)
                return_copy(c).start()

        def own(c, carry):
            cols = ds(c * PANEL, PANEL)
            xbuf[:, cols] = advanced(t_ref, xbuf, cols)
            return carry

        lax.fori_loop(0, count, own, 0)
        if phase != DOWN:
            for c in range(max(count - 2, 0), count):
                return_copy(c).wait_send()
            waited(xr.at[:, pl.ds(0, w)], xrecv.at[phase])

        def weights(k, weight, weight_new, kind, first=None):
            buf = wrow if kind == 'rows' else wcol
            count = w // 256

            def part(ref, i):
                if kind == 'rows':
                    return ref.at[ds(i * 256, 256), :]
                return ref.at[:, ds(i * 256, 256)]

            def load(i):
                return pltpu.make_async_copy(part(weight, i), buf.at[lax.rem(i, 3)], wl_sem.at[lax.rem(i, 3)])

            def store(i):
                return pltpu.make_async_copy(buf.at[lax.rem(i, 3)], part(weight_new, i), ws_sem.at[lax.rem(i, 3)])

            load(jnp.int32(0)).start()
            load(jnp.int32(1)).start()

            def one(i, carry):
                cols = ds(i * 256, 256)
                slot = lax.rem(i, 3)
                load(i).wait()

                def put(x_orth):
                    buf[slot] = weight_step(buf[slot], x_orth.T if kind == 'rows' else x_orth, scale)

                if phase == DOWN:
                    put(xbuf[:, cols].astype(F32))
                else:
                    @pl.when(core == k)
                    def _():
                        put(xbuf[:, cols].astype(F32))

                    @pl.when(core != k)
                    def _():
                        put(xr[:, cols])
                store(i).start()

                @pl.when(i >= 1)
                def _():
                    store(i - 1).wait()

                @pl.when(i + 2 < count)
                def _():
                    load(i + 2).start()
                if first is not None:
                    @pl.when(lax.rem(i, 3) == 2)
                    def _():
                        service(first + lax.div(i, 3), first, first + 1)
                return carry

            lax.fori_loop(0, count, one, 0)
            store(jnp.int32(count - 1)).wait()

        return weights

    load_grads(jnp.int32(0), 0, 0)
    load_grads(jnp.int32(1), 1, 1)
    services(0, 19)
    w_long, w_mid = w_gate.shape[1], w_o.shape[0]

    def scale_of(w):
        return 0.2 * math.sqrt(max(d, 2 * w))

    weights = newton(DOWN, w_long, scale_of(w_long), 20)
    weights(0, w_down, wn_down, 'rows', 30)
    services(32, 43)
    weights = newton(GATE_UP, w_long, scale_of(w_long), 44)
    weights(0, w_gate, wn_gate, 'cols', 54)
    weights(1, w_up, wn_up, 'cols')
    services(56, 59)
    newton(O_Q, w_mid, scale_of(w_mid), 60)
    handed = [pltpu.make_async_copy(xbuf.at[:, pl.ds(0, w_mid)], own_out, wl_sem.at[0]),
              pltpu.make_async_copy(xr.at[:, pl.ds(0, w_mid)], other_out, wl_sem.at[1])]
    for copy in handed:
        copy.start()
    services(70, PAIRS + 7)
    normalize(KEY_VALUE, 2 * GROUP_COLS, sb_ref)
    handed.append(pltpu.make_async_copy(sb_ref, kv_out, kv_sem))
    handed[-1].start()
    for slot in range(4):
        for k in range(2):
            waited(mst.at[slot, k], ms_sem.at[slot, k])
    for copy in handed:
        copy.wait()


def main_step(grads, weights, moms):
    any_spec = pl.BlockSpec(memory_space=pl.ANY)
    ins = list(grads) + list(weights) + list(moms)
    d, width = weights[0].shape
    outs = [jax.ShapeDtypeStruct(a.shape, F32) for a in list(weights[2:]) + list(moms)] + [
        jax.ShapeDtypeStruct((d, d), BF16), jax.ShapeDtypeStruct((d, weights[1].shape[0]), BF16),
        jax.ShapeDtypeStruct((d, weights[1].shape[0]), F32)]
    w_long = weights[2].shape[1]
    dma = pltpu.SemaphoreType.DMA
    pieces = (PIECE_R, PIECE_C)
    return pl.pallas_call(
        step_kernel,
        out_shape=outs,
        in_specs=[any_spec] * len(ins),
        out_specs=[any_spec] * len(outs),
        scratch_shapes=[
            pltpu.VMEM((2, d, w_long), F32), pltpu.VMEM((d, 2 * w_long), BF16), pltpu.VMEM((d, d), F32), pltpu.VMEM((d, d), BF16),
            pltpu.VMEM((d, d), BF16), pltpu.VMEM((d, w_long), F32), pltpu.VMEM((3, 256, d), F32), pltpu.VMEM((3, d, 256), F32),
            pltpu.VMEM((4, 2, HALF_R, PIECE_C), F32), pltpu.VMEM((4, 2, HALF_R, PIECE_C), F32),
            pltpu.VMEM((8, 2, HALF_R, PIECE_C), F32), pltpu.VMEM((8, 2, QUART_R, PIECE_C), F32), pltpu.VMEM((8, 2) + pieces, F32),
            pltpu.VMEM((8, 2) + pieces, BF16), pltpu.VMEM((4, 2) + pieces, F32), pltpu.VMEM((4, 2) + pieces, F32),
            pltpu.VMEM((2,) + pieces, F32), pltpu.VMEM((2, PIECE_C, PIECE_R), F32),
            dma((8, 2)), dma((4, 2)), dma((4, 2)), dma((4, 2)), dma((4, 2)), dma((8, 2)), dma((8, 2)), dma((8, 2)),
            dma((8, 2)), dma((8, 2)), dma((8, 2)), dma((8, 2)), dma((8, 2)),
            dma((2,)), dma, dma((4,)), dma((2,)), dma((3,)), dma((3,)), dma((3,)), dma, pltpu.SemaphoreType.REGULAR],
        compiler_params=pltpu.CompilerParams(vmem_limit_bytes=VMEM_BYTES, collective_id=0, has_side_effects=True),
        cost_estimate=pl.CostEstimate(flops=10 ** 11, bytes_accessed=2 * 10 ** 8, transcendentals=0),
    )(*ins)


def update_other(weight, x_back, weight_new, scale, core):
    rows, width = x_back.shape
    theirs = pl.BlockSpec((rows, HEAD_DIM), lambda g, c: (0, 4 * g + 3 - c[0]))

    def body(c_ref, w_ref, back_ref, unused, o_ref):
        o_ref[...] = weight_step(w_ref[...], back_ref[...], scale)

    moved = 12 * rows * width
    return pl.pallas_call(
        body, out_shape=jax.ShapeDtypeStruct(weight.shape, F32),
        grid_spec=pltpu.PrefetchScalarGridSpec(
            num_scalar_prefetch=1, grid=(width // HEAD_DIM,),
            in_specs=[theirs, pl.BlockSpec((rows, HEAD_DIM), lambda g, c: (0, g)), pl.BlockSpec(memory_space=pl.ANY)],
            out_specs=theirs),
        input_output_aliases={3: 0},
        compiler_params=pltpu.CompilerParams(vmem_limit_bytes=VMEM_BYTES),
        cost_estimate=pl.CostEstimate(flops=moved, bytes_accessed=moved, transcendentals=0),
    )(core, weight, x_back, weight_new)


def finish_kernel(*refs):
    x_in, own_in, other_in, w_qkv, w_o = refs[:5]
    srcs, out_far, wn_qkv, wn_o, dsts = refs[5:13], refs[13], refs[14], refs[15], refs[16:24]
    x_ref, x_own, s_ref, sb_ref, t_ref, wk = refs[24:30]
    bufs = refs[30:36]
    in_sem, out_sem, wl_sem, ws_sem, x_sem, step_sem, done_sem = refs[36:]
    d, w = out_far.shape
    load = pltpu.make_async_copy(x_in, x_ref, x_sem)
    load.start()
    core = lax.axis_index('tp')
    heads = [(g * HEAD_DIM, ds((4 * g + 2 + core) * HEAD_DIM, HEAD_DIM)) for g in range(w // HEAD_DIM)]
    scale = 0.2 * math.sqrt(max(d, 2 * w))
    for lo, at in heads:
        pltpu.make_async_copy(w_qkv.at[:, at], wk.at[:, lo:lo + HEAD_DIM], wl_sem).start()

    square = [buf.at[:d, :d] for buf in bufs]
    w_o_buf, w_q_buf, x_other = square[3:]
    queries = [(slice(g * GROUP_COLS, (g + 1) * GROUP_COLS), slice(2 * g * GROUP_COLS, (2 * g + 1) * GROUP_COLS))
               for g in range(d // GROUP_COLS)]
    moves = [(srcs[n], dsts[n]) for n in (2, 7, 0, 5, 1, 6, 4)] + [(srcs[3].at[:, lo:lo + d], dsts[3].at[:, lo:lo + d]) for lo in (0, d)]
    step_scale = 0.2 * math.sqrt(max(d, 2 * x_own.shape[1]))

    def held(n):
        return bufs[n] if n < 6 else square[n - 6]

    def fetch(n):
        if n >= 6:
            put_copy(n - 6).wait()
        pltpu.make_async_copy(moves[n][0], held(n), in_sem.at[n]).start()

    def put_copy(n):
        return pltpu.make_async_copy(held(n), moves[n][1], out_sem.at[n])

    def put(n):
        pltpu.make_async_copy(moves[n][0], held(n), in_sem.at[n]).wait()
        put_copy(n).start()

    for n in range(3):
        fetch(n)
    loads = [pltpu.make_async_copy(other_in, x_other, step_sem.at[0]), pltpu.make_async_copy(own_in, x_own, step_sem.at[1]),
             pltpu.make_async_copy(w_o, w_o_buf, step_sem.at[2])]
    for copy in loads:
        copy.start()
    for near, at in queries:
        pltpu.make_async_copy(w_qkv.at[:, at], w_q_buf.at[:, near], step_sem.at[3]).start()

    def panels(mine, one):
        def loop(read):
            def body(c, carry):
                cols = ds(c * GROUP_COLS, GROUP_COLS)
                one(cols, read(cols))
                return carry
            lax.fori_loop(0, d // GROUP_COLS, body, 0)
        pl.when(core == mine)(lambda: loop(lambda cols: x_own[:, cols].astype(F32)))
        pl.when(core != mine)(lambda: loop(lambda cols: x_other[:, cols]))

    def step_o(unused):
        for copy in loads:
            copy.wait()

        def one(rows, x_orth):
            w_o_buf[rows, :] = weight_step(w_o_buf[rows, :], x_orth.T, step_scale)
        panels(0, one)
        pltpu.make_async_copy(w_o_buf, wn_o, done_sem.at[0]).start()

    def step_q(unused):
        pltpu.make_async_copy(w_q_buf, w_q_buf, step_sem.at[3]).wait()

        def one(cols, x_orth):
            w_q_buf[:, cols] = weight_step(w_q_buf[:, cols], x_orth, step_scale)
        panels(1, one)
        for near, at in queries:
            pltpu.make_async_copy(w_q_buf.at[:, near], wn_qkv.at[:, at], done_sem.at[1]).start()

    def freed(which):
        pltpu.make_async_copy((w_o_buf, w_q_buf)[which], (w_o_buf, w_q_buf)[which], done_sem.at[which]).wait()

    plan = {(0, 1): ((put, 0),), (0, 2): ((put, 1),), (1, 0): ((put, 2), (fetch, 6)), (1, 1): ((fetch, 7),),
            (1, 2): ((put, 6), (fetch, 8)), (2, 0): ((put, 7), (step_o, 0)), (2, 1): ((step_q, 0), (fetch, 5), (put, 8)),
            (2, 2): ((freed, 0), (fetch, 3)), (3, 0): ((freed, 1), (fetch, 4)), (3, 1): ((put, 5),), (3, 2): ((put, 3),),
            (4, 0): ((put, 4),)}

    def step(i, carry):
        def at(slot):
            for turn in range(NEWTON_STEPS):
                if (turn, slot) in plan:
                    @pl.when(i == turn)
                    def _(todo=plan[turn, slot]):
                        for act, n in todo:
                            act(n)

        at(0)
        gram_step(x_ref, 2 * w, s_ref, sb_ref, BLOCK)
        at(1)
        poly_step(s_ref, sb_ref, t_ref, BLOCK)
        at(2)

        @pl.when(i < NEWTON_STEPS - 1)
        def _():
            def move(c, inner):
                cols = ds(c * PANEL, PANEL)
                x_ref[:, cols] = advanced(t_ref, x_ref, cols)
                return inner
            lax.fori_loop(0, 2 * w // PANEL, move, 0)
        return carry

    load.wait()
    lax.fori_loop(0, NEWTON_STEPS, step, 0)
    for c in range(w // PANEL):
        cols = slice(c * PANEL, (c + 1) * PANEL)
        out_far[:, cols] = advanced(t_ref, x_ref, pl.ds(w + c * PANEL, PANEL)).astype(F32)
    pltpu.make_async_copy(wk, wk, wl_sem).wait()
    for c in range(w // PANEL):
        cols = slice(c * PANEL, (c + 1) * PANEL)
        wk[:, cols] = weight_step(wk[:, cols], advanced(t_ref, x_ref, pl.ds(c * PANEL, PANEL)).astype(F32), scale)
    for lo, at in heads:
        pltpu.make_async_copy(wk.at[:, lo:lo + HEAD_DIM], wn_qkv.at[:, at], ws_sem).start()
    for n in range(3, 9):
        put_copy(n).wait()
    pltpu.make_async_copy(wk, wk, ws_sem).wait()


def finish(handed, w_qkv, w_o, arrays):
    d = handed[0].shape[0]
    w = handed[0].shape[1] // 2
    ins = list(handed) + [w_qkv, w_o] + list(arrays)
    any_spec = pl.BlockSpec(memory_space=pl.ANY)
    vmem = pl.BlockSpec(memory_space=pltpu.VMEM)
    dma = pltpu.SemaphoreType.DMA
    outs = [jax.ShapeDtypeStruct((d, w), F32)] + [jax.ShapeDtypeStruct(a.shape, F32) for a in [w_qkv, w_o] + list(arrays)]
    return pl.pallas_call(
        finish_kernel,
        out_shape=outs,
        in_specs=[any_spec] * len(ins),
        out_specs=[vmem] + [any_spec] * (len(outs) - 1),
        scratch_shapes=[pltpu.VMEM((d, d), BF16), pltpu.VMEM(handed[1].shape, BF16), pltpu.VMEM((d, d), F32), pltpu.VMEM((d, d), BF16),
                        pltpu.VMEM((d, d), BF16), pltpu.VMEM((d, w), F32)]
        + [pltpu.VMEM(arrays[n].shape, F32) for n in (2, 7, 0, 5, 1, 6)]
        + [dma((9,)), dma((9,)), dma, dma, dma, dma((4,)), dma((2,))],
        compiler_params=pltpu.CompilerParams(vmem_limit_bytes=VMEM_BYTES),
        cost_estimate=pl.CostEstimate(flops=3 * 10 ** 10, bytes_accessed=12 * 10 ** 7, transcendentals=0),
    )(*ins)


def solution(mesh):
    tp_count = mesh.shape['tp']
    col_spec = P(None, 'tp')
    row_spec = P('tp', None)
    grad_col = P('dp', None, 'tp')
    grad_row = P('dp', 'tp', None)
    weight_specs = (col_spec, row_spec, col_spec, col_spec, row_spec)
    in_specs = (grad_col, grad_row, grad_col, grad_col, grad_row) + weight_specs + weight_specs
    out_specs = weight_specs + weight_specs
    swap = [(0, 1), (1, 0)]

    def local_step(*arrays):
        weights, moms = arrays[5:10], arrays[10:]
        results = main_step([block[0] for block in arrays[:5]], weights, moms)
        done = finish(results[8:], weights[0], weights[1], results[:8])
        x_far, done = done[0], list(done[1:])
        scale = 0.2 * math.sqrt(max(x_far.shape[0], x_far.shape[1] * tp_count))
        core = lax.axis_index('tp').astype(jnp.int32).reshape(1)
        done[0] = update_other(weights[0], lax.ppermute(x_far, 'tp', swap), done[0], scale, core)
        return tuple(done)

    return jax.shard_map(local_step, mesh=mesh, in_specs=in_specs, out_specs=out_specs, check_vma=False)
```
